256 devices in a mesh: batch: 16 (over y_lo, z), head: 16 (over y_hi, x, core).
Axes of the slice: x: 4, y: 4 (y_hi: 2, y_lo: 2; y = y_hi * 2 + y_lo), z: 8, core: 2. Of those that a mesh axis runs over, the one named last changes fastest.
Arguments:
- latent_codes: int32 [16, 2048, 576], P('batch', 'head'), may hold values from -127 to 127
- exponents: int32 [16, 2048], P('batch', 'head'), may hold values from -9 to -5
- lengths: int32 [16], P('batch'), may hold values from 512 to 2048, as said below
- queries: bfloat16 [16, 128, 24576], P('batch', 'head'), may hold values from -30000 to 30000
- out_grad: bfloat16 [16, 128, 16384], P('batch', 'head'), may hold values from -24 to 24
- w_key: bfloat16 [512, 16384], P(None, 'head'), may hold values from -0.25 to 0.25
- w_value: bfloat16 [512, 16384], P(None, 'head'), may hold values from -0.25 to 0.25
Outputs:
- latent_grad: float32 [16, 2048, 576], P('batch', 'head')
- key_weight_grad: float32 [512, 16384], P(None, 'head')
- value_weight_grad: float32 [512, 16384], P(None, 'head')
The draws below stay inside these ranges and needn't reach their ends.
Inputs may be any that keep to these rules, and one draw needn't show every extreme that they name: Rows j of group g with j < lengths[g] are live; some group uses the whole prefix.
All inputs are finite; a program needn't handle non-finite values.
Results may differ from the reference program's by a relative error of at most 0.04.
Values may be sent and summed in bfloat16 or wider, within the bound.
No kernel may reach another device: no remote copies, remote signals or barrier semaphores. Data moves between devices by JAX's collectives and lax.ppermute only.
A program may use at most 128 MiB of HBM per device.

```python
import jax
import jax.numpy as jnp
import numpy as np
from jax import lax

LATENT = 512
ROPE = 64
NOPE = 128
VHEAD = 128
HEADS = 128
PREFIX = 2048
QUERIES = 128
GROUPS = 16


def shared_integers(key):
    latent_codes = jax.random.randint(jax.random.fold_in(key, 11), (GROUPS, PREFIX, LATENT + ROPE), -127, 128, dtype=jnp.int32)
    exponents = jax.random.randint(jax.random.fold_in(key, 12), (GROUPS, PREFIX), -9, -4, dtype=jnp.int32)
    lengths = jax.random.randint(jax.random.fold_in(key, 13), (GROUPS,), PREFIX // 4, PREFIX + 1, dtype=jnp.int32)
    full_group = jax.random.randint(jax.random.fold_in(key, 14), (), 0, GROUPS, dtype=jnp.int32)
    short_step = jax.random.randint(jax.random.fold_in(key, 15), (), 0, GROUPS - 1, dtype=jnp.int32)
    short_group = (full_group + 1 + short_step) % GROUPS
    group_index = jnp.arange(GROUPS, dtype=jnp.int32)
    lengths = jnp.where(group_index == full_group, PREFIX, lengths)
    lengths = jnp.where(group_index == short_group, PREFIX // 4, lengths)
    return (latent_codes, exponents, lengths)


def draw_latent_codes(key, part):
    return shared_integers(key)[0]


def draw_exponents(key, part):
    return shared_integers(key)[1]


def draw_lengths(key, part):
    return shared_integers(key)[2]


def draw_queries(key, part):
    shape = (GROUPS, QUERIES, HEADS, NOPE + ROPE)
    drawn = jnp.clip(3.0 * jax.random.normal(jax.random.fold_in(key, 21), shape, jnp.float32), -18.0, 18.0)
    return drawn.reshape(GROUPS, QUERIES, HEADS * (NOPE + ROPE)).astype(jnp.bfloat16)


def shard_levels(own_key, extent, pieces, least, largest):
    factor_of, own = 1.0, jax.random.fold_in(own_key, 6)
    for dim, shards_of in pieces:
        draws = jnp.exp(jax.random.uniform(jax.random.fold_in(own, dim), (shards_of,), jnp.float32, least / len(pieces), largest / len(pieces)))
        factor_of = factor_of * jnp.repeat(draws, extent[dim] // shards_of).reshape([-1 if axis == dim else 1 for axis in range(len(extent))])
    return factor_of


def noise(stream_key, dims, scale, most, cuts=(), kind=jnp.bfloat16):
    result = scale * jax.random.normal(stream_key, dims, jnp.float32)
    if cuts:
        result = result * shard_levels(stream_key, dims, cuts, -0.22, 0.18)
    return jnp.clip(result, -most, most).astype(kind)


def setup_inputs(seed: int = 0) -> dict:
    seeds = jax.random.split(jax.random.key(seed), 8)
    return {
        "latent_codes": draw_latent_codes(jax.random.fold_in(seeds[7], 71), 0),
        "exponents": draw_exponents(jax.random.fold_in(seeds[7], 71), 0),
        "lengths": draw_lengths(jax.random.fold_in(seeds[7], 71), 0),
        "queries": draw_queries(jax.random.fold_in(seeds[7], 71), 0),
        "out_grad": noise(seeds[4], (GROUPS, QUERIES, HEADS * VHEAD), 4.0, 24.0, ((0, 16), (1, 16))),
        "w_key": noise(seeds[5], (LATENT, HEADS * NOPE), LATENT ** -0.5, 0.25, ((1, 16),)),
        "w_value": noise(seeds[6], (LATENT, HEADS * VHEAD), LATENT ** -0.5, 0.25, ((1, 16),)),
    }


lower_exponent = -9


def dequantize(latent_codes, exponents):
    levels = jnp.arange(5, dtype=jnp.int32) + lower_exponent
    powers = jnp.asarray(np.array([2.0 ** level for level in range(-9, -4)]), jnp.float32)
    factor = jnp.sum(jnp.where(exponents[..., None] == levels, powers, jnp.float32(0.0)), axis=-1)
    return (latent_codes.astype(jnp.float32) * factor[..., None]).astype(jnp.bfloat16)


def one_group(latent, length, query_rows, grad_rows, w_key, w_value):
    score_scale = (NOPE + ROPE) ** -0.5
    lat_main = latent[:, :LATENT]
    lat_rope = latent[:, LATENT:]
    key_rows = jnp.dot(lat_main, w_key, preferred_element_type=jnp.float32).astype(jnp.bfloat16).reshape(PREFIX, HEADS, NOPE)
    value_rows = jnp.dot(lat_main, w_value, preferred_element_type=jnp.float32).astype(jnp.bfloat16).reshape(PREFIX, HEADS, VHEAD)
    query_all = query_rows.reshape(QUERIES, HEADS, NOPE + ROPE).astype(jnp.float32)
    q_nope = query_all[..., :NOPE]
    q_rope = query_all[..., NOPE:]
    scores = jnp.einsum("qhd,khd->hqk", q_nope, key_rows.astype(jnp.float32))
    scores = (scores + jnp.einsum("qhd,kd->hqk", q_rope, lat_rope.astype(jnp.float32))) * score_scale
    usable = jnp.arange(PREFIX, dtype=jnp.int32) < length
    scores = jnp.where(usable, scores, -jnp.inf)
    row_top = jnp.max(scores, axis=-1, keepdims=True)
    expd = jnp.exp(scores - row_top)
    probs = expd / jnp.sum(expd, axis=-1, keepdims=True)
    low_probs = probs.astype(jnp.bfloat16).astype(jnp.float32)
    values_f = value_rows.astype(jnp.float32)
    attended = jnp.einsum("hqk,khd->qhd", low_probs, values_f).astype(jnp.bfloat16)
    grad_heads = grad_rows.reshape(QUERIES, HEADS, VHEAD).astype(jnp.float32)
    out_dot = jnp.sum(grad_heads * attended.astype(jnp.float32), axis=-1)
    grad_probs = jnp.einsum("qhd,khd->hqk", grad_heads, values_f)
    grad_scores = (score_scale * probs * (grad_probs - out_dot.T[:, :, None])).astype(jnp.bfloat16).astype(jnp.float32)
    grad_values = jnp.einsum("hqk,qhd->khd", low_probs, grad_heads).astype(jnp.bfloat16).reshape(PREFIX, HEADS * VHEAD)
    grad_keys = jnp.einsum("hqk,qhd->khd", grad_scores, q_nope).astype(jnp.bfloat16).reshape(PREFIX, HEADS * NOPE)
    grad_rope = jnp.einsum("hqk,qhd->kd", grad_scores, q_rope)
    main_grad = jnp.dot(grad_values, w_value.T, preferred_element_type=jnp.float32)
    main_grad = main_grad + jnp.dot(grad_keys, w_key.T, preferred_element_type=jnp.float32)
    latent_grad = jnp.concatenate([main_grad, grad_rope], axis=1)
    key_part = jnp.dot(lat_main.T, grad_keys, preferred_element_type=jnp.float32)
    value_part = jnp.dot(lat_main.T, grad_values, preferred_element_type=jnp.float32)
    return latent_grad, key_part, value_part


def reference(latent_codes, exponents, lengths, queries, out_grad, w_key, w_value):
    latent = dequantize(latent_codes, exponents)

    def step(carry, inputs):
        latent_one, length, query_rows, grad_rows = inputs
        latent_grad, key_part, value_part = one_group(latent_one, length, query_rows, grad_rows, w_key, w_value)
        return (carry[0] + key_part, carry[1] + value_part), latent_grad

    start = (jnp.zeros((LATENT, HEADS * NOPE), jnp.float32), jnp.zeros((LATENT, HEADS * VHEAD), jnp.float32))
    sums, latent_grad = lax.scan(step, start, (latent, lengths, queries, out_grad))
    return latent_grad, sums[0], sums[1]
```

```python
import jax
import jax.numpy as jnp
import numpy as np
from jax import lax
from jax.experimental import pallas as pl
from jax.experimental.pallas import tpu as pltpu
from jax.sharding import Mesh
from jax.sharding import PartitionSpec as P

LATENT = 512
ROPE = 64
NOPE = 128
VHEAD = 128
FEATURES = NOPE + ROPE
SCALE = FEATURES ** (-0.5)
LOG2E = float(np.log2(np.e))
QUERIES = 128
PAIR = 2
ROWS = PAIR * QUERIES
BLOCK = 16


lower_exponent = -9


def dequantize_columns(codes, exponents):
    levels = jnp.arange(5, dtype=jnp.int32) + lower_exponent
    powers = jnp.asarray(np.array([2.0**level for level in range(-9, -4)]), jnp.float32)
    factor = jnp.sum(jnp.where(exponents[..., None] == levels, powers, jnp.float32(0.0)), axis=-1)
    return (codes.astype(jnp.float32) * factor[None, :]).astype(jnp.bfloat16)


def dot_nn(left, right):
    return lax.dot_general(
        left, right, (((1,), (0,)), ((), ())), preferred_element_type=jnp.float32
    )


def dot_nt(left, right):
    return lax.dot_general(
        left, right, (((1,), (1,)), ((), ())), preferred_element_type=jnp.float32
    )


def heads_kernel(
    bias_ref, own_ref, other_ref, q_ref, g_ref, wk_ref, wv_ref,
    grads_ref, low_ref, ds_ref, qa_ref, ga_ref,
    scores_ref, gp_ref,
):
    bf16 = jnp.bfloat16
    half = own_ref.shape[1]
    sides = ((own_ref, slice(0, half)), (other_ref, slice(half, 2 * half)))
    eye = (
        lax.broadcasted_iota(jnp.int32, (ROPE, ROPE), 0)
        == lax.broadcasted_iota(jnp.int32, (ROPE, ROPE), 1)
    ).astype(jnp.float32).astype(bf16)
    q_rows, r_rows, g_rows = [], [], []
    for h in range(PAIR):
        start = h * FEATURES
        nope = q_ref[:, start : start + NOPE]
        rope = q_ref[:, start + NOPE : start + FEATURES]
        grad = g_ref[:, h * VHEAD : (h + 1) * VHEAD]
        wk = wk_ref[:, h * NOPE : (h + 1) * NOPE]
        wv = wv_ref[:, h * VHEAD : (h + 1) * VHEAD]
        q_rows.append(dot_nt(nope, wk).astype(bf16))
        r_rows.append(rope)
        g_rows.append(dot_nt(grad, wv).astype(bf16))
        columns = slice(h * QUERIES, (h + 1) * QUERIES)
        qa_ref[:LATENT, columns] = dot_nt(wk, nope).astype(bf16)
        qa_ref[LATENT:, columns] = dot_nt(eye, rope).astype(bf16)
        ga_ref[:, columns] = dot_nt(wv, grad).astype(bf16)
    q_all = jnp.concatenate(q_rows, axis=0)
    r_all = jnp.concatenate(r_rows, axis=0)
    g_all = jnp.concatenate(g_rows, axis=0)
    for lat_ref, columns in sides:
        scores_ref[:, columns] = dot_nn(q_all, lat_ref[:LATENT, :]) + dot_nn(
            r_all, lat_ref[LATENT:, :]
        )
        gp_ref[:, columns] = dot_nn(g_all, lat_ref[:LATENT, :])

    def softmax_rows(step, carry):
        rows = pl.ds(pl.multiple_of(step * BLOCK, BLOCK), BLOCK)
        shifted = scores_ref[rows, :] + bias_ref[...]
        top = jnp.max(shifted, axis=1, keepdims=True)
        expd = jnp.exp2((shifted - top) * (SCALE * LOG2E))
        probs = expd * (1.0 / jnp.sum(expd, axis=1, keepdims=True))
        low = probs.astype(bf16)
        low_ref[rows, :] = low
        gp = gp_ref[rows, :]
        out_dot = jnp.sum(low.astype(jnp.float32) * gp, axis=1, keepdims=True)
        ds_ref[rows, :] = (SCALE * probs * (gp - out_dot)).astype(bf16)
        return carry

    lax.fori_loop(0, ROWS // BLOCK, softmax_rows, 0)

    def back(rows_ref):
        total = dot_nt(own_ref[:LATENT, :], rows_ref[:, :half])
        return (total + dot_nt(other_ref[:LATENT, :], rows_ref[:, half:])).astype(bf16)

    back_k, back_v = back(ds_ref), back(low_ref)
    for h in range(PAIR):
        start = h * FEATURES
        columns = slice(h * QUERIES, (h + 1) * QUERIES)
        grads_ref[0, :, columns] = dot_nn(
            back_k[:, columns], q_ref[:, start : start + NOPE]
        ).astype(bf16)
        grads_ref[1, :, columns] = dot_nn(
            back_v[:, columns], g_ref[:, h * VHEAD : (h + 1) * VHEAD]
        ).astype(bf16)


def heads_call(bias, own, other, qg, wk, wv, first, pairs):
    total = pairs * ROWS
    half = own.shape[1]
    prefix = 2 * half
    skip = wk.shape[1] * FEATURES // (NOPE * PAIR * VHEAD)
    flops = 2 * total * prefix * LATENT * 4
    return pl.pallas_call(
        heads_kernel,
        grid=(pairs,),
        in_specs=[
            pl.BlockSpec((1, prefix), lambda p: (0, 0)),
            pl.BlockSpec((LATENT + ROPE, half), lambda p: (0, 0)),
            pl.BlockSpec((LATENT + ROPE, half), lambda p: (0, 0)),
            pl.BlockSpec((QUERIES, PAIR * FEATURES), lambda p: (0, first + p)),
            pl.BlockSpec((QUERIES, PAIR * VHEAD), lambda p: (0, skip + first + p)),
            pl.BlockSpec((LATENT, PAIR * NOPE), lambda p: (0, first + p)),
            pl.BlockSpec((LATENT, PAIR * VHEAD), lambda p: (0, first + p)),
        ],
        out_specs=[
            pl.BlockSpec((2, LATENT, PAIR * NOPE), lambda p: (0, 0, p)),
            pl.BlockSpec((ROWS, prefix), lambda p: (p, 0)),
            pl.BlockSpec((ROWS, prefix), lambda p: (p, 0)),
            pl.BlockSpec((LATENT + ROPE, ROWS), lambda p: (0, p)),
            pl.BlockSpec((LATENT, ROWS), lambda p: (0, p)),
        ],
        out_shape=[
            jax.ShapeDtypeStruct((2, LATENT, pairs * PAIR * NOPE), jnp.bfloat16),
            jax.ShapeDtypeStruct((total, prefix), jnp.bfloat16),
            jax.ShapeDtypeStruct((total, prefix), jnp.bfloat16),
            jax.ShapeDtypeStruct((LATENT + ROPE, total), jnp.bfloat16),
            jax.ShapeDtypeStruct((LATENT, total), jnp.bfloat16),
        ],
        scratch_shapes=[
            pltpu.VMEM((ROWS, prefix), jnp.float32),
            pltpu.VMEM((ROWS, prefix), jnp.float32),
        ],
        compiler_params=pltpu.CompilerParams(
            dimension_semantics=("arbitrary",), vmem_limit_bytes=30 * 1024 * 1024
        ),
        cost_estimate=pl.CostEstimate(
            flops=flops, bytes_accessed=8 * 1024 * 1024, transcendentals=total * prefix
        ),
        name="heads",
    )(bias, own, other, qg, qg, wk, wv)


def latent_kernel(qa0_ref, qa1_ref, ga0_ref, ga1_ref, ds0_ref, ds1_ref, low0_ref, low1_ref, out_ref):
    value = dot_nn(ga0_ref[...], low0_ref[...]) + dot_nn(ga1_ref[...], low1_ref[...])
    key = dot_nn(qa0_ref[:LATENT, :], ds0_ref[...]) + dot_nn(qa1_ref[:LATENT, :], ds1_ref[...])
    out_ref[:LATENT, :] = (value + key).astype(jnp.bfloat16)
    out_ref[LATENT:, :] = (
        dot_nn(qa0_ref[LATENT:, :], ds0_ref[...]) + dot_nn(qa1_ref[LATENT:, :], ds1_ref[...])
    ).astype(jnp.bfloat16)


def latent_call(first, second, side):
    (_, low0, ds0, qa0, ga0), (_, low1, ds1, qa1, ga1) = first, second
    prefix = low0.shape[1] // 2
    total = low0.shape[0]
    tile = 256
    skip = side * prefix // tile
    whole = lambda array: pl.BlockSpec(array.shape, lambda t: (0, 0))
    columns = pl.BlockSpec((total, tile), lambda t: (0, skip + t))
    return pl.pallas_call(
        latent_kernel,
        grid=(prefix // tile,),
        in_specs=[whole(qa0), whole(qa1), whole(ga0), whole(ga1)] + [columns] * 4,
        out_specs=pl.BlockSpec((LATENT + ROPE, tile), lambda t: (0, t)),
        out_shape=jax.ShapeDtypeStruct((LATENT + ROPE, prefix), jnp.bfloat16),
        compiler_params=pltpu.CompilerParams(
            dimension_semantics=("arbitrary",), vmem_limit_bytes=24 * 1024 * 1024
        ),
        cost_estimate=pl.CostEstimate(
            flops=2 * 2 * 2 * total * prefix * LATENT, bytes_accessed=12 * 1024 * 1024, transcendentals=0
        ),
        name="latent_rows",
    )(qa0, qa1, ga0, ga1, ds0, ds1, low0, low1)


OFFSETS = (0, 1, -1, 2, -2, 3, -3, 4)


def assemble_kernel(index_ref, *refs):
    place = index_ref[0]
    depth = len(OFFSETS)
    pieces = refs[:depth]
    key_ref, value_ref = refs[depth:]
    shard = pieces[0].shape[1] // 4
    width = pieces[0].shape[2]
    for k, offset in enumerate(OFFSETS):
        z = lax.rem(place - offset + depth, depth)
        low = pl.ds(pl.multiple_of(z * shard, shard), shard)
        high = pl.ds(pl.multiple_of((depth + z) * shard, shard), shard)
        both = pl.ds(pl.multiple_of(z * 2 * shard, 2 * shard), 2 * shard)
        for part, out_ref in enumerate((key_ref, value_ref)):
            piece = pieces[k]
            out_ref[low, :width] = piece[part, :shard].astype(jnp.float32)
            out_ref[high, :width] = piece[part, shard : 2 * shard].astype(jnp.float32)
            out_ref[both, width:] = piece[part, 2 * shard :].astype(jnp.float32)


def assemble_call(place, pieces):
    vmem = pl.BlockSpec(memory_space=pltpu.VMEM)
    out = jax.ShapeDtypeStruct((LATENT, 2 * pieces[0].shape[2]), jnp.float32)
    return pl.pallas_call(
        assemble_kernel,
        in_specs=[pl.BlockSpec(memory_space=pltpu.SMEM)] + [vmem] * len(pieces),
        out_specs=[vmem, vmem],
        out_shape=[out, out],
        compiler_params=pltpu.CompilerParams(vmem_limit_bytes=16 * 1024 * 1024),
        cost_estimate=pl.CostEstimate(flops=1 << 20, bytes_accessed=6 * 1024 * 1024, transcendentals=0),
        name="assemble",
    )(place, *pieces)


def ring(size, shift):
    return [(i, (i + shift) % size) for i in range(size)]


def wide_add(*terms):
    total = terms[0].astype(jnp.float32)
    for term in terms[1:]:
        total = total + term.astype(jnp.float32)
    return total


def tie(value, *others):
    return lax.optimization_barrier((value, *others))


def reduce_ring(take, axis, fillers):
    size = lax.axis_size(axis)
    ahead = size // 2
    behind = size - 1 - ahead
    right, left = take(ahead), take(-behind)
    filled = []
    for step in range(ahead):
        right = lax.ppermute(right, axis, ring(size, 1))
        if step < behind:
            left = lax.ppermute(left, axis, ring(size, -1))
        if step < len(fillers):
            done = fillers[step]()
            right, done = tie(right, done)
            filled.append(done)
        if step < ahead - 1:
            right = wide_add(right, take(ahead - 1 - step)).astype(jnp.bfloat16)
        if step < behind - 1:
            left = wide_add(left, take(-behind + 1 + step)).astype(jnp.bfloat16)
    return wide_add(right, left, take(0)).astype(jnp.bfloat16), filled


def gather_ring(shard, axis):
    size = lax.axis_size(axis)
    ahead = size // 2
    parts = {0: shard}
    right = left = shard
    for step in range(1, ahead + 1):
        right = lax.ppermute(right, axis, ring(size, 1))
        parts[step] = right
        if step < ahead:
            left = lax.ppermute(left, axis, ring(size, -1))
            parts[-step] = left
    return [parts[offset] for offset in OFFSETS]


def swap(value, axis):
    return lax.ppermute(value, axis, ring(2, 1))


def per_device(latent_codes, exponents, lengths, queries, out_grad, w_key, w_value):
    bf16 = jnp.bfloat16
    ny, nx = lax.axis_size("yh"), lax.axis_size("x")
    chips = ny * nx
    y, x, c = lax.axis_index("yh"), lax.axis_index("x"), lax.axis_index("core")
    yl, z = lax.axis_index("yl"), lax.axis_index("z")
    shifts = [0, 1, nx - 1] + list(range(2, nx - 1))
    rows = latent_codes.shape[1]
    tokens = queries.shape[1]

    local = dequantize_columns(latent_codes[0].T, exponents[0])
    both_y = jnp.concatenate([local, swap(local, "yh")], axis=1)
    lat_parts = [lax.ppermute(both_y, "x", ring(nx, b)) if b else both_y for b in shifts]
    own = jnp.concatenate(lat_parts, axis=1)
    other = swap(own, "core")

    def by_core(core):
        blocks = []
        for array in (queries, out_grad):
            width = array.shape[2] // (2 * chips)
            block = array[0].reshape(tokens, ny, nx, 2, width)
            blocks.append(lax.dynamic_index_in_dim(block, core, 3, keepdims=False))
        return jnp.concatenate(blocks, axis=3)

    qg = jnp.concatenate([by_core(c), swap(by_core(1 - c), "core")], axis=0)
    qg_parts = []
    for b in shifts:
        part = lax.dynamic_index_in_dim(qg, lax.rem(x + b, nx), 2, keepdims=False)
        qg_parts.append(lax.ppermute(part, "x", ring(nx, b)) if b else part)
    qg = jnp.concatenate(qg_parts, axis=0)
    qg_keep = lax.dynamic_index_in_dim(qg, y, 1, keepdims=False)
    qg_give = lax.dynamic_index_in_dim(qg, 1 - y, 1, keepdims=False)
    qg = jnp.concatenate([qg_keep, swap(qg_give, "yh")], axis=0)

    def row_starts(core):
        return [
            ((lax.rem(y + a, ny) * nx + lax.rem(x - b + nx, nx)) * 2 + core) * rows
            for b in shifts
            for a in range(ny)
        ]

    starts = jnp.stack(row_starts(c) + row_starts(1 - c))
    positions = (starts[:, None] + jnp.arange(rows, dtype=jnp.int32)[None, :]).reshape(1, -1)
    bias = jnp.where(positions < lengths[0], jnp.float32(0.0), -jnp.inf)

    pairs = w_key.shape[1] // (2 * PAIR * NOPE)
    first = heads_call(bias, own, other, qg, w_key, w_value, 0, pairs)
    second = heads_call(bias, own, other, qg, w_key, w_value, pairs, pairs)

    nz = lax.axis_size("z")
    half = LATENT // 2
    keep = lax.dynamic_slice_in_dim(first[0], yl * half, half, 1)
    give = lax.dynamic_slice_in_dim(first[0], (1 - yl) * half, half, 1)
    sum_a = wide_add(keep, swap(give, "yl")).astype(bf16)
    shard = half // nz
    pieces_a = sum_a.reshape(2, nz, shard, -1)
    pieces_b = second[0].reshape(2, nz, 2 * shard, -1)

    def take(offset):
        place = lax.rem(z + offset + nz, nz)
        return jnp.concatenate(
            [lax.dynamic_index_in_dim(p, place, 1, keepdims=False) for p in (pieces_a, pieces_b)], axis=1
        )

    summed, (far, near) = reduce_ring(
        take, "z", (lambda: latent_call(first, second, 1), lambda: latent_call(first, second, 0))
    )
    partner = swap(summed, "yl")
    own_a, other_a = summed[:, :shard], partner[:, :shard]
    low_a = jnp.where(yl == 0, own_a, other_a)
    high_a = jnp.where(yl == 0, other_a, own_a)
    sum_b = wide_add(summed[:, shard:], partner[:, shard:]).astype(bf16)
    pieces = gather_ring(jnp.concatenate([low_a, high_a, sum_b], axis=1), "z")

    pair_sum = wide_add(near, swap(far, "core")).astype(bf16)
    width = ny * rows
    back = []
    for k, b in enumerate(shifts):
        part = pair_sum[:, k * width : (k + 1) * width]
        back.append(lax.ppermute(part, "x", ring(nx, -b)) if b else part)
    row_sum = wide_add(*back)
    latent_grad = row_sum[:, :rows] + swap(row_sum[:, rows:].astype(bf16), "yh").astype(jnp.float32)

    key_sum, value_sum = assemble_call(z[None].astype(jnp.int32), pieces)
    return (latent_grad.T[None], key_sum, value_sum)


def solution(mesh):
    devices = mesh.devices.reshape(2, 8, 2, 4, 2)
    split = Mesh(devices, ("yl", "z", "yh", "x", "core"))
    batch, head = ("yl", "z"), ("yh", "x", "core")
    in_specs = (
        P(batch, head, None),
        P(batch, head),
        P(batch),
        P(batch, head, None),
        P(batch, head, None),
        P(None, head),
        P(None, head),
    )
    out_specs = (P(batch, head, None), P(None, head), P(None, head))
    return jax.shard_map(
        per_device, mesh=split, in_specs=in_specs, out_specs=out_specs, check_vma=False
    )
```

```python
import functools

import jax
import jax.numpy as jnp
import numpy as np
from jax import lax
from jax.experimental import pallas as pl
from jax.experimental.pallas import tpu as pltpu
from jax.sharding import Mesh
from jax.sharding import PartitionSpec as P

LATENT = 512
ROPE = 64
NOPE = 128
VHEAD = 128
FEATURES = NOPE + ROPE
SCALE = FEATURES ** (-0.5)
LOG2E = float(np.log2(np.e))
QUERIES = 128
PAIR = 4
ROWS = PAIR * QUERIES
BLOCK = 16
LANES = 128


lower_exponent = -9


def dequantize_columns(codes, exponents):
    levels = jnp.arange(5, dtype=jnp.int32) + lower_exponent
    powers = jnp.asarray(np.array([2.0**level for level in range(-9, -4)]), jnp.float32)
    factor = jnp.sum(jnp.where(exponents[..., None] == levels, powers, jnp.float32(0.0)), axis=-1)
    return (codes.astype(jnp.float32) * factor[None, :]).astype(jnp.bfloat16)


def dot_nn(left, right):
    return lax.dot_general(
        left, right, (((1,), (0,)), ((), ())), preferred_element_type=jnp.float32
    )


def dot_nt(left, right):
    return lax.dot_general(
        left, right, (((1,), (1,)), ((), ())), preferred_element_type=jnp.float32
    )


def heads_kernel(
    first, pairs,
    bias_ref, own_ref, other_ref, qg_ref, wk_ref, wv_ref,
    grads_ref, low_ref, ds_ref, qa_ref, ga_ref,
    scores_ref, gp_ref, top_ref, sum_ref, mix_ref,
):
    bf16 = jnp.bfloat16
    half = own_ref.shape[1]
    skip = qg_ref.shape[1] * FEATURES // (FEATURES + VHEAD)
    sides = ((own_ref, slice(0, half)), (other_ref, slice(half, 2 * half)))
    eye = (
        lax.broadcasted_iota(jnp.int32, (ROPE, ROPE), 0)
        == lax.broadcasted_iota(jnp.int32, (ROPE, ROPE), 1)
    ).astype(jnp.float32).astype(bf16)

    def one_pair(pair, carry):
        def window(width, extra=0):
            return pl.ds(pl.multiple_of(extra + (first + pair) * width, 128), width)

        q_pair = qg_ref[:, window(PAIR * FEATURES)]
        g_pair = qg_ref[:, window(PAIR * VHEAD, skip)]
        wk_pair = wk_ref[:, window(PAIR * NOPE)]
        wv_pair = wv_ref[:, window(PAIR * VHEAD)]
        q_rows, r_rows, g_rows, nopes, grads = [], [], [], [], []
        qa_columns, ga_columns = [], []
        for h in range(PAIR):
            start = h * FEATURES
            nope = q_pair[:, start : start + NOPE]
            rope = q_pair[:, start + NOPE : start + FEATURES]
            grad = g_pair[:, h * VHEAD : (h + 1) * VHEAD]
            wk = wk_pair[:, h * NOPE : (h + 1) * NOPE]
            wv = wv_pair[:, h * VHEAD : (h + 1) * VHEAD]
            q_rows.append(dot_nt(nope, wk).astype(bf16))
            r_rows.append(rope)
            g_rows.append(dot_nt(grad, wv).astype(bf16))
            nopes.append(nope)
            grads.append(grad)
            columns = pl.ds(pl.multiple_of((pair * PAIR + h) * QUERIES, QUERIES), QUERIES)
            qa_ref[:LATENT, columns] = dot_nt(wk, nope).astype(bf16)
            qa_ref[LATENT:, columns] = dot_nt(eye, rope).astype(bf16)
            ga_ref[:, columns] = dot_nt(wv, grad).astype(bf16)
        q_all = jnp.concatenate(q_rows, axis=0)
        r_all = jnp.concatenate(r_rows, axis=0)
        g_all = jnp.concatenate(g_rows, axis=0)
        for lat_ref, columns in sides:
            scores_ref[:, columns] = (
                dot_nn(q_all, lat_ref[:LATENT, :])
                + dot_nn(r_all, lat_ref[LATENT:, :])
                + bias_ref[:, columns]
            )
            gp_ref[:, columns] = dot_nn(g_all, lat_ref[:LATENT, :])

        blocks = ROWS // BLOCK
        lanes = [slice(LANES * j, LANES * (j + 1)) for j in range(2 * half // LANES)]

        def row_block(step):
            return pl.ds(pl.multiple_of(step * BLOCK, BLOCK), BLOCK)

        def find_top(step, carry):
            rows = row_block(step)
            tops = [scores_ref[rows, lane] for lane in lanes]
            while len(tops) > 1:
                tops = [jnp.maximum(u, v) for u, v in zip(tops[::2], tops[1::2])]
            top_ref[rows, :] = tops[0]
            return carry

        lax.fori_loop(0, blocks, find_top, 0, unroll=2)
        top = jnp.max(top_ref[...], axis=1, keepdims=True)
        top_ref[...] = jnp.broadcast_to(top, top_ref.shape)

        def exponentiate(step, carry):
            rows = row_block(step)
            top = top_ref[rows, :]
            total = mixed = None
            for lane in lanes:
                expd = jnp.exp2((scores_ref[rows, lane] - top) * (SCALE * LOG2E))
                scores_ref[rows, lane] = expd
                product = expd * gp_ref[rows, lane]
                total = expd if total is None else total + expd
                mixed = product if mixed is None else mixed + product
            sum_ref[rows, :] = total
            mix_ref[rows, :] = mixed
            return carry

        lax.fori_loop(0, blocks, exponentiate, 0, unroll=2)
        inverse = 1.0 / jnp.sum(sum_ref[...], axis=1, keepdims=True)
        out_dot = jnp.sum(mix_ref[...], axis=1, keepdims=True) * inverse
        sum_ref[...] = jnp.broadcast_to(inverse, sum_ref.shape)
        mix_ref[...] = jnp.broadcast_to(out_dot, mix_ref.shape)

        def finish(step, carry):
            rows = row_block(step)
            place = pl.ds(pl.multiple_of(pair * ROWS + step * BLOCK, BLOCK), BLOCK)
            inverse, out_dot = sum_ref[rows, :], mix_ref[rows, :]
            for lane in lanes:
                probs = scores_ref[rows, lane] * inverse
                low_ref[place, lane] = probs.astype(bf16)
                ds_ref[place, lane] = (probs * SCALE * (gp_ref[rows, lane] - out_dot)).astype(bf16)
            return carry

        lax.fori_loop(0, blocks, finish, 0, unroll=2)
        rows = pl.ds(pl.multiple_of(pair * ROWS, ROWS), ROWS)

        def back(rows_ref):
            total = dot_nt(own_ref[:LATENT, :], rows_ref[rows, :half])
            return (total + dot_nt(other_ref[:LATENT, :], rows_ref[rows, half:])).astype(bf16)

        back_k, back_v = back(ds_ref), back(low_ref)
        for h in range(PAIR):
            columns = slice(h * QUERIES, (h + 1) * QUERIES)
            place = pl.ds(pl.multiple_of((pair * PAIR + h) * NOPE, NOPE), NOPE)
            grads_ref[0, :, place] = dot_nn(back_k[:, columns], nopes[h]).astype(bf16)
            grads_ref[1, :, place] = dot_nn(back_v[:, columns], grads[h]).astype(bf16)
        return carry

    lax.fori_loop(0, pairs, one_pair, 0)


def heads_call(bias, own, other, qg, wk, wv, first, pairs):
    total = pairs * ROWS
    prefix = 2 * own.shape[1]
    flops = 2 * total * prefix * LATENT * 4
    vmem = pl.BlockSpec(memory_space=pltpu.VMEM)
    return pl.pallas_call(
        functools.partial(heads_kernel, first, pairs),
        in_specs=[vmem] * 6,
        out_specs=[vmem] * 5,
        out_shape=[
            jax.ShapeDtypeStruct((2, LATENT, pairs * PAIR * NOPE), jnp.bfloat16),
            jax.ShapeDtypeStruct((total, prefix), jnp.bfloat16),
            jax.ShapeDtypeStruct((total, prefix), jnp.bfloat16),
            jax.ShapeDtypeStruct((LATENT + ROPE, total), jnp.bfloat16),
            jax.ShapeDtypeStruct((LATENT, total), jnp.bfloat16),
        ],
        scratch_shapes=[
            pltpu.VMEM((ROWS, prefix), jnp.float32),
            pltpu.VMEM((ROWS, prefix), jnp.float32),
            pltpu.VMEM((ROWS, LANES), jnp.float32),
            pltpu.VMEM((ROWS, LANES), jnp.float32),
            pltpu.VMEM((ROWS, LANES), jnp.float32),
        ],
        compiler_params=pltpu.CompilerParams(vmem_limit_bytes=24 * 1024 * 1024),
        cost_estimate=pl.CostEstimate(
            flops=flops, bytes_accessed=8 * 1024 * 1024, transcendentals=total * prefix
        ),
        name="heads",
    )(bias, own, other, qg, wk, wv)


def latent_kernel(start, qa0_ref, qa1_ref, ga0_ref, ga1_ref, ds0_ref, ds1_ref, low0_ref, low1_ref, out_ref):
    tile = 256

    def one_tile(step, carry):
        source = pl.ds(pl.multiple_of(start + step * tile, tile), tile)
        place = pl.ds(pl.multiple_of(step * tile, tile), tile)
        ds0, ds1 = ds0_ref[:, source], ds1_ref[:, source]
        value = dot_nn(ga0_ref[...], low0_ref[:, source]) + dot_nn(ga1_ref[...], low1_ref[:, source])
        key = dot_nn(qa0_ref[:LATENT, :], ds0) + dot_nn(qa1_ref[:LATENT, :], ds1)
        out_ref[:LATENT, place] = (value + key).astype(jnp.bfloat16)
        out_ref[LATENT:, place] = (
            dot_nn(qa0_ref[LATENT:, :], ds0) + dot_nn(qa1_ref[LATENT:, :], ds1)
        ).astype(jnp.bfloat16)
        return carry

    lax.fori_loop(0, out_ref.shape[1] // tile, one_tile, 0)


def latent_call(first, second, side):
    (_, low0, ds0, qa0, ga0), (_, low1, ds1, qa1, ga1) = first, second
    prefix = low0.shape[1] // 2
    total = low0.shape[0]
    vmem = pl.BlockSpec(memory_space=pltpu.VMEM)
    return pl.pallas_call(
        functools.partial(latent_kernel, side * prefix),
        in_specs=[vmem] * 8,
        out_specs=vmem,
        out_shape=jax.ShapeDtypeStruct((LATENT + ROPE, prefix), jnp.bfloat16),
        compiler_params=pltpu.CompilerParams(vmem_limit_bytes=24 * 1024 * 1024),
        cost_estimate=pl.CostEstimate(
            flops=2 * 2 * 2 * total * prefix * LATENT, bytes_accessed=12 * 1024 * 1024, transcendentals=0
        ),
        name="latent_rows",
    )(qa0, qa1, ga0, ga1, ds0, ds1, low0, low1)


OFFSETS = (0, 1, -1, 2, -2, 3, -3, 4)


def assemble_kernel(index_ref, *refs):
    side, place = index_ref[0], index_ref[1]
    depth = len(OFFSETS)
    pieces = refs[:depth]
    key_ref, value_ref = refs[depth:]
    shard = pieces[0].shape[1] // 4
    width = pieces[0].shape[2]
    for k, offset in enumerate(OFFSETS):
        z = lax.rem(place - offset + depth, depth)
        kept = pl.ds(pl.multiple_of((side * depth + z) * shard, shard), shard)
        given = pl.ds(pl.multiple_of(((1 - side) * depth + z) * shard, shard), shard)
        both = pl.ds(pl.multiple_of(z * 2 * shard, 2 * shard), 2 * shard)
        for part, out_ref in enumerate((key_ref, value_ref)):
            piece = pieces[k]
            out_ref[kept, :width] = piece[part, :shard].astype(jnp.float32)
            out_ref[given, :width] = piece[part, shard : 2 * shard].astype(jnp.float32)
            out_ref[both, width:] = piece[part, 2 * shard :].astype(jnp.float32)


def assemble_call(place, pieces):
    vmem = pl.BlockSpec(memory_space=pltpu.VMEM)
    out = jax.ShapeDtypeStruct((LATENT, 2 * pieces[0].shape[2]), jnp.float32)
    return pl.pallas_call(
        assemble_kernel,
        in_specs=[pl.BlockSpec(memory_space=pltpu.SMEM)] + [vmem] * len(pieces),
        out_specs=[vmem, vmem],
        out_shape=[out, out],
        compiler_params=pltpu.CompilerParams(vmem_limit_bytes=16 * 1024 * 1024),
        cost_estimate=pl.CostEstimate(flops=1 << 20, bytes_accessed=6 * 1024 * 1024, transcendentals=0),
        name="assemble",
    )(place, *pieces)


def ring(size, shift):
    return [(i, (i + shift) % size) for i in range(size)]


def wide_add(*terms):
    total = terms[0].astype(jnp.float32)
    for term in terms[1:]:
        total = total + term.astype(jnp.float32)
    return total


def tie(value, *others):
    return lax.optimization_barrier((value, *others))


def reduce_ring(take, axis, fillers):
    size = lax.axis_size(axis)
    ahead = size // 2
    behind = size - 1 - ahead
    right, left = take(ahead), take(-behind)
    filled = []
    for step in range(ahead):
        ready = right
        right = lax.ppermute(right, axis, ring(size, 1))
        if step < behind:
            left = lax.ppermute(left, axis, ring(size, -1))
        if step < len(fillers):
            done = fillers[step](ready)
            right, done = tie(right, done)
            filled.append(done)
        if step < ahead - 1:
            right = wide_add(right, take(ahead - 1 - step)).astype(jnp.bfloat16)
        if step < behind - 1:
            left = wide_add(left, take(-behind + 1 + step)).astype(jnp.bfloat16)
    return wide_add(right, left, take(0)).astype(jnp.bfloat16), filled


def gather_ring(shard, axis):
    size = lax.axis_size(axis)
    ahead = size // 2
    parts = {0: shard}
    right = left = shard
    for step in range(1, ahead + 1):
        right = lax.ppermute(right, axis, ring(size, 1))
        parts[step] = right
        if step < ahead:
            left = lax.ppermute(left, axis, ring(size, -1))
            parts[-step] = left
    return [parts[offset] for offset in OFFSETS]


def swap(value, axis):
    return lax.ppermute(value, axis, ring(2, 1))


def per_device(latent_codes, exponents, lengths, queries, out_grad, w_key, w_value):
    bf16 = jnp.bfloat16
    ny, nx = lax.axis_size("yh"), lax.axis_size("x")
    chips = ny * nx
    y, x, c = lax.axis_index("yh"), lax.axis_index("x"), lax.axis_index("core")
    yl, z = lax.axis_index("yl"), lax.axis_index("z")
    shifts = [0, 1, nx - 1] + list(range(2, nx - 1))
    rows = latent_codes.shape[1]
    tokens = queries.shape[1]

    def by_core(core):
        blocks = []
        for array in (queries, out_grad):
            width = array.shape[2] // (2 * chips)
            block = array[0].reshape(tokens, ny, nx, 2, width)
            blocks.append(lax.dynamic_index_in_dim(block, core, 3, keepdims=False))
        return jnp.concatenate(blocks, axis=3)

    qg_away = by_core(1 - c)
    codes, qg_away = tie(latent_codes, qg_away)
    local = dequantize_columns(codes[0].T, exponents[0])
    both_y = jnp.concatenate([local, swap(local, "yh")], axis=1)
    qg = jnp.concatenate([by_core(c), swap(qg_away, "core")], axis=0)
    qg_parts = [lax.dynamic_index_in_dim(qg, lax.rem(x + b, nx), 2, keepdims=False) for b in shifts]
    both_y, *qg_parts = tie(both_y, *qg_parts)
    qg_parts = [lax.ppermute(part, "x", ring(nx, b)) if b else part for part, b in zip(qg_parts, shifts)]
    lat_parts = [lax.ppermute(both_y, "x", ring(nx, b)) if b else both_y for b in shifts]
    own = jnp.concatenate(lat_parts, axis=1)
    other = swap(own, "core")

    qg = jnp.concatenate(qg_parts, axis=0)
    qg_keep = lax.dynamic_index_in_dim(qg, y, 1, keepdims=False)
    qg_give = lax.dynamic_index_in_dim(qg, 1 - y, 1, keepdims=False)
    qg = jnp.concatenate([qg_keep, swap(qg_give, "yh")], axis=0)

    def row_starts(core):
        return [
            ((lax.rem(y + a, ny) * nx + lax.rem(x - b + nx, nx)) * 2 + core) * rows
            for b in shifts
            for a in range(ny)
        ]

    starts = jnp.stack(row_starts(c) + row_starts(1 - c))
    positions = (starts[:, None] + jnp.arange(rows, dtype=jnp.int32)[None, :]).reshape(1, -1)
    bias = jnp.where(positions < lengths[0], jnp.float32(0.0), -jnp.inf)

    pairs = w_key.shape[1] // (2 * PAIR * NOPE)
    first = heads_call(bias, own, other, qg, w_key, w_value, 0, pairs)
    second = heads_call(bias, own, other, qg, w_key, w_value, pairs, pairs)

    nz = lax.axis_size("z")
    half = LATENT // 2
    keep = lax.dynamic_slice_in_dim(first[0], yl * half, half, 1)
    give = lax.dynamic_slice_in_dim(first[0], (1 - yl) * half, half, 1)
    sum_a = wide_add(keep, swap(give, "yl")).astype(bf16)
    shard = half // nz
    pieces_a = sum_a.reshape(2, nz, shard, -1)
    pieces_b = second[0].reshape(2, nz, 2 * shard, -1)

    def take(offset):
        place = lax.rem(z + offset + nz, nz)
        return jnp.concatenate(
            [lax.dynamic_index_in_dim(p, place, 1, keepdims=False) for p in (pieces_a, pieces_b)], axis=1
        )

    def row_grads(side):
        return lambda ready: latent_call(first, tie(second, ready)[0], side)

    summed, (far, near) = reduce_ring(take, "z", (row_grads(1), row_grads(0)))
    partner = swap(summed, "yl")
    sum_b = wide_add(summed[:, shard:], partner[:, shard:]).astype(bf16)
    pieces = gather_ring(jnp.concatenate([summed[:, :shard], partner[:, :shard], sum_b], axis=1), "z")

    pair_sum = wide_add(near, swap(far, "core")).astype(bf16)
    width = ny * rows
    back = []
    for k, b in enumerate(shifts):
        part = pair_sum[:, k * width : (k + 1) * width]
        back.append(lax.ppermute(part, "x", ring(nx, -b)) if b else part)
    row_sum = wide_add(*back)
    latent_grad = row_sum[:, :rows] + swap(row_sum[:, rows:].astype(bf16), "yh").astype(jnp.float32)

    key_sum, value_sum = assemble_call(jnp.stack([yl, z]).astype(jnp.int32), pieces)
    return (latent_grad.T[None], key_sum, value_sum)


def solution(mesh):
    devices = mesh.devices.reshape(2, 8, 2, 4, 2)
    split = Mesh(devices, ("yl", "z", "yh", "x", "core"))
    batch, head = ("yl", "z"), ("yh", "x", "core")
    in_specs = (
        P(batch, head, None),
        P(batch, head),
        P(batch),
        P(batch, head, None),
        P(batch, head, None),
        P(None, head),
        P(None, head),
    )
    out_specs = (P(batch, head, None), P(None, head), P(None, head))
    return jax.shard_map(
        per_device, mesh=split, in_specs=in_specs, out_specs=out_specs, check_vma=False
    )
```

```python
import functools

import jax
import jax.numpy as jnp
import numpy as np
from jax import lax
from jax.experimental import pallas as pl
from jax.experimental.pallas import tpu as pltpu
from jax.sharding import Mesh
from jax.sharding import PartitionSpec as P

LATENT = 512
ROPE = 64
NOPE = 128
VHEAD = 128
FEATURES = NOPE + ROPE
SCALE = FEATURES ** (-0.5)
LOG2E = float(np.log2(np.e))
QUERIES = 128
PAIR = 4
ROWS = PAIR * QUERIES
BLOCK = 16
LANES = 128


lower_exponent = -9


def dequantize_columns(codes, exponents):
    levels = jnp.arange(5, dtype=jnp.int32) + lower_exponent
    powers = jnp.asarray(np.array([2.0**level for level in range(-9, -4)]), jnp.float32)
    factor = jnp.sum(jnp.where(exponents[..., None] == levels, powers, jnp.float32(0.0)), axis=-1)
    return (codes.astype(jnp.float32) * factor[None, :]).astype(jnp.bfloat16)


def dot_nn(left, right):
    return lax.dot_general(
        left, right, (((1,), (0,)), ((), ())), preferred_element_type=jnp.float32
    )


def dot_nt(left, right):
    return lax.dot_general(
        left, right, (((1,), (1,)), ((), ())), preferred_element_type=jnp.float32
    )


def project_kernel(qg_ref, wk_ref, wv_ref, qa_ref, ra_ref, ga_ref, qt_ref, gt_ref):
    bf16 = jnp.bfloat16
    eye = (
        lax.broadcasted_iota(jnp.int32, (ROPE, ROPE), 0)
        == lax.broadcasted_iota(jnp.int32, (ROPE, ROPE), 1)
    ).astype(jnp.float32).astype(bf16)
    pairs = wk_ref.shape[1] // (2 * NOPE)
    skip = wk_ref.shape[1] * FEATURES // NOPE

    def one_pair(pair, carry):
        def window(width, extra=0):
            return pl.ds(pl.multiple_of(extra + pair * width, 128), width)

        q_pair = qg_ref[:, window(2 * FEATURES)]
        for h in range(2):
            nope = q_pair[:, h * FEATURES : h * FEATURES + NOPE]
            rope = q_pair[:, h * FEATURES + NOPE : (h + 1) * FEATURES]
            head = pl.ds(pl.multiple_of((2 * pair + h) * NOPE, NOPE), NOPE)
            grad = qg_ref[:, pl.ds(pl.multiple_of(skip + (2 * pair + h) * VHEAD, VHEAD), VHEAD)]
            wk, wv = wk_ref[:, head], wv_ref[:, head]
            qa_ref[head, :] = dot_nt(nope, wk).astype(bf16)
            ra_ref[head, :] = rope
            ga_ref[head, :] = dot_nt(grad, wv).astype(bf16)
            qt_ref[:LATENT, head] = dot_nt(wk, nope).astype(bf16)
            qt_ref[LATENT:, head] = dot_nt(eye, rope).astype(bf16)
            gt_ref[:, head] = dot_nt(wv, grad).astype(bf16)
        return carry

    lax.fori_loop(0, pairs, one_pair, 0)


def project_call(qg, wk, wv):
    total = wk.shape[1] // NOPE * QUERIES
    vmem = pl.BlockSpec(memory_space=pltpu.VMEM)
    shapes = [(total, LATENT), (total, ROPE), (total, LATENT), (LATENT + ROPE, total), (LATENT, total)]
    return pl.pallas_call(
        project_kernel,
        in_specs=[vmem] * 3,
        out_specs=[vmem] * 5,
        out_shape=[jax.ShapeDtypeStruct(shape, jnp.bfloat16) for shape in shapes],
        compiler_params=pltpu.CompilerParams(vmem_limit_bytes=16 * 1024 * 1024),
        cost_estimate=pl.CostEstimate(
            flops=40 * 4 * total * NOPE * LATENT, bytes_accessed=8 * 1024 * 1024, transcendentals=0
        ),
        name="project",
    )(qg, wk, wv)


def heads_kernel(
    first, pairs,
    bias_ref, own_ref, other_ref, qg_ref, qa_ref, ra_ref, ga_ref,
    grads_ref, low_ref, ds_ref,
    scores_ref, gp_ref, top_ref, sum_ref, mix_ref,
):
    bf16 = jnp.bfloat16
    half = own_ref.shape[1]
    skip = qg_ref.shape[1] * FEATURES // (FEATURES + VHEAD)
    sides = ((own_ref, slice(0, half)), (other_ref, slice(half, 2 * half)))

    def one_pair(pair, carry):
        def window(width, extra=0):
            return pl.ds(pl.multiple_of(extra + (first + pair) * width, 128), width)

        q_pair = qg_ref[:, window(PAIR * FEATURES)]
        g_pair = qg_ref[:, window(PAIR * VHEAD, skip)]
        nopes = [q_pair[:, h * FEATURES : h * FEATURES + NOPE] for h in range(PAIR)]
        grads = [g_pair[:, h * VHEAD : (h + 1) * VHEAD] for h in range(PAIR)]
        here = window(ROWS)
        q_all, r_all, g_all = qa_ref[here, :], ra_ref[here, :], ga_ref[here, :]
        for lat_ref, columns in sides:
            scores_ref[:, columns] = (
                dot_nn(q_all, lat_ref[:LATENT, :])
                + dot_nn(r_all, lat_ref[LATENT:, :])
                + bias_ref[:, columns]
            )
            gp_ref[:, columns] = dot_nn(g_all, lat_ref[:LATENT, :])

        blocks = ROWS // BLOCK
        lanes = [slice(LANES * j, LANES * (j + 1)) for j in range(2 * half // LANES)]

        def row_block(step):
            return pl.ds(pl.multiple_of(step * BLOCK, BLOCK), BLOCK)

        def find_top(step, carry):
            rows = row_block(step)
            tops = [scores_ref[rows, lane] for lane in lanes]
            while len(tops) > 1:
                tops = [jnp.maximum(u, v) for u, v in zip(tops[::2], tops[1::2])]
            top_ref[rows, :] = tops[0]
            return carry

        lax.fori_loop(0, blocks, find_top, 0, unroll=2)
        top = jnp.max(top_ref[...], axis=1, keepdims=True)
        top_ref[...] = jnp.broadcast_to(top, top_ref.shape)

        def exponentiate(step, carry):
            rows = row_block(step)
            top = top_ref[rows, :]
            total = mixed = None
            for lane in lanes:
                expd = jnp.exp2((scores_ref[rows, lane] - top) * (SCALE * LOG2E))
                scores_ref[rows, lane] = expd
                product = expd * gp_ref[rows, lane]
                total = expd if total is None else total + expd
                mixed = product if mixed is None else mixed + product
            sum_ref[rows, :] = total
            mix_ref[rows, :] = mixed
            return carry

        lax.fori_loop(0, blocks, exponentiate, 0, unroll=2)
        inverse = 1.0 / jnp.sum(sum_ref[...], axis=1, keepdims=True)
        out_dot = jnp.sum(mix_ref[...], axis=1, keepdims=True) * inverse
        sum_ref[...] = jnp.broadcast_to(inverse, sum_ref.shape)
        mix_ref[...] = jnp.broadcast_to(out_dot, mix_ref.shape)

        def finish(step, carry):
            rows = row_block(step)
            place = pl.ds(pl.multiple_of(pair * ROWS + step * BLOCK, BLOCK), BLOCK)
            inverse, out_dot = sum_ref[rows, :], mix_ref[rows, :]
            for lane in lanes:
                probs = scores_ref[rows, lane] * inverse
                low_ref[place, lane] = probs.astype(bf16)
                ds_ref[place, lane] = (probs * SCALE * (gp_ref[rows, lane] - out_dot)).astype(bf16)
            return carry

        lax.fori_loop(0, blocks, finish, 0, unroll=2)
        rows = pl.ds(pl.multiple_of(pair * ROWS, ROWS), ROWS)

        def back(rows_ref):
            total = dot_nt(own_ref[:LATENT, :], rows_ref[rows, :half])
            return (total + dot_nt(other_ref[:LATENT, :], rows_ref[rows, half:])).astype(bf16)

        back_k, back_v = back(ds_ref), back(low_ref)
        for h in range(PAIR):
            columns = slice(h * QUERIES, (h + 1) * QUERIES)
            place = pl.ds(pl.multiple_of((pair * PAIR + h) * NOPE, NOPE), NOPE)
            grads_ref[0, :, place] = dot_nn(back_k[:, columns], nopes[h]).astype(bf16)
            grads_ref[1, :, place] = dot_nn(back_v[:, columns], grads[h]).astype(bf16)
        return carry

    lax.fori_loop(0, pairs, one_pair, 0)


def heads_call(bias, own, other, qg, projected, first, pairs):
    total = pairs * ROWS
    prefix = 2 * own.shape[1]
    flops = 2 * total * prefix * LATENT * 4
    vmem = pl.BlockSpec(memory_space=pltpu.VMEM)
    return pl.pallas_call(
        functools.partial(heads_kernel, first, pairs),
        in_specs=[vmem] * 7,
        out_specs=[vmem] * 3,
        out_shape=[
            jax.ShapeDtypeStruct((2, LATENT, pairs * PAIR * NOPE), jnp.bfloat16),
            jax.ShapeDtypeStruct((total, prefix), jnp.bfloat16),
            jax.ShapeDtypeStruct((total, prefix), jnp.bfloat16),
        ],
        scratch_shapes=[
            pltpu.VMEM((ROWS, prefix), jnp.float32),
            pltpu.VMEM((ROWS, prefix), jnp.float32),
            pltpu.VMEM((ROWS, LANES), jnp.float32),
            pltpu.VMEM((ROWS, LANES), jnp.float32),
            pltpu.VMEM((ROWS, LANES), jnp.float32),
        ],
        compiler_params=pltpu.CompilerParams(vmem_limit_bytes=24 * 1024 * 1024),
        cost_estimate=pl.CostEstimate(
            flops=flops, bytes_accessed=8 * 1024 * 1024, transcendentals=total * prefix
        ),
        name="heads",
    )(bias, own, other, qg, *projected)


def latent_kernel(start, qt_ref, gt_ref, ds0_ref, ds1_ref, low0_ref, low1_ref, out_ref):
    tile = 256
    total = ds0_ref.shape[0]

    def one_tile(step, carry):
        source = pl.ds(pl.multiple_of(start + step * tile, tile), tile)
        place = pl.ds(pl.multiple_of(step * tile, tile), tile)
        ds0, ds1 = ds0_ref[:, source], ds1_ref[:, source]
        value = dot_nn(gt_ref[:, :total], low0_ref[:, source]) + dot_nn(
            gt_ref[:, total:], low1_ref[:, source]
        )
        key = dot_nn(qt_ref[:LATENT, :total], ds0) + dot_nn(qt_ref[:LATENT, total:], ds1)
        out_ref[:LATENT, place] = (value + key).astype(jnp.bfloat16)
        out_ref[LATENT:, place] = (
            dot_nn(qt_ref[LATENT:, :total], ds0) + dot_nn(qt_ref[LATENT:, total:], ds1)
        ).astype(jnp.bfloat16)
        return carry

    lax.fori_loop(0, out_ref.shape[1] // tile, one_tile, 0)


def latent_call(transposed, first, second, side):
    (_, low0, ds0), (_, low1, ds1) = first, second
    prefix = low0.shape[1] // 2
    total = low0.shape[0]
    vmem = pl.BlockSpec(memory_space=pltpu.VMEM)
    return pl.pallas_call(
        functools.partial(latent_kernel, side * prefix),
        in_specs=[vmem] * 6,
        out_specs=vmem,
        out_shape=jax.ShapeDtypeStruct((LATENT + ROPE, prefix), jnp.bfloat16),
        compiler_params=pltpu.CompilerParams(vmem_limit_bytes=24 * 1024 * 1024),
        cost_estimate=pl.CostEstimate(
            flops=2 * 2 * 2 * total * prefix * LATENT, bytes_accessed=12 * 1024 * 1024, transcendentals=0
        ),
        name="latent_rows",
    )(*transposed, ds0, ds1, low0, low1)


OFFSETS = (0, 1, -1, 2, -2, 3, -3, 4)


def assemble_kernel(index_ref, *refs):
    side, place = index_ref[0], index_ref[1]
    depth = len(OFFSETS)
    shard = refs[0].shape[0] // 4
    width = refs[0].shape[1]
    for k, offset in enumerate(OFFSETS):
        z = lax.rem(place - offset + depth, depth)
        kept = pl.ds(pl.multiple_of((side * depth + z) * shard, shard), shard)
        given = pl.ds(pl.multiple_of(((1 - side) * depth + z) * shard, shard), shard)
        both = pl.ds(pl.multiple_of(z * 2 * shard, 2 * shard), 2 * shard)
        for part, out_ref in enumerate(refs[2 * depth :]):
            piece = refs[part * depth + k]
            out_ref[kept, :width] = piece[:shard, :].astype(jnp.float32)
            out_ref[given, :width] = piece[shard : 2 * shard, :].astype(jnp.float32)
            out_ref[both, width:] = piece[2 * shard :, :].astype(jnp.float32)


def assemble_call(place, pieces):
    vmem = pl.BlockSpec(memory_space=pltpu.VMEM)
    out = jax.ShapeDtypeStruct((LATENT, 2 * pieces[0].shape[1]), jnp.float32)
    return pl.pallas_call(
        assemble_kernel,
        in_specs=[pl.BlockSpec(memory_space=pltpu.SMEM)] + [vmem] * len(pieces),
        out_specs=[vmem, vmem],
        out_shape=[out, out],
        compiler_params=pltpu.CompilerParams(vmem_limit_bytes=16 * 1024 * 1024),
        cost_estimate=pl.CostEstimate(flops=1 << 20, bytes_accessed=6 * 1024 * 1024, transcendentals=0),
        name="assemble",
    )(place, *pieces)


def ring(size, shift):
    return [(i, (i + shift) % size) for i in range(size)]


def wide_add(*terms):
    total = terms[0].astype(jnp.float32)
    for term in terms[1:]:
        total = total + term.astype(jnp.float32)
    return total


def tie(value, *others):
    return lax.optimization_barrier((value, *others))


def reduce_ring(take, axis, fillers):
    size = lax.axis_size(axis)
    ahead = size // 2
    behind = size - 1 - ahead
    right, left = take(ahead), take(-behind)
    filled = []
    for step in range(ahead):
        ready = right
        right = lax.ppermute(right, axis, ring(size, 1))
        if step < behind:
            left = lax.ppermute(left, axis, ring(size, -1))
        if step < len(fillers):
            done = fillers[step](ready)
            right = tie(right, done)[0]
            filled.append(done)
        if step < ahead - 1:
            right = wide_add(right, take(ahead - 1 - step)).astype(jnp.bfloat16)
        if step < behind - 1:
            left = wide_add(left, take(-behind + 1 + step)).astype(jnp.bfloat16)
    return wide_add(right, left, take(0)).astype(jnp.bfloat16), filled


def gather_ring(shard, axis):
    size = lax.axis_size(axis)
    ahead = size // 2
    parts = {0: shard}
    right = left = shard
    for step in range(1, ahead + 1):
        right = lax.ppermute(right, axis, ring(size, 1))
        parts[step] = right
        if step < ahead:
            left = lax.ppermute(left, axis, ring(size, -1))
            parts[-step] = left
    return [parts[offset] for offset in OFFSETS]


def swap(value, axis):
    return lax.ppermute(value, axis, ring(2, 1))


def per_device(latent_codes, exponents, lengths, queries, out_grad, w_key, w_value):
    bf16 = jnp.bfloat16
    ny, nx = lax.axis_size("yh"), lax.axis_size("x")
    chips = ny * nx
    y, x, c = lax.axis_index("yh"), lax.axis_index("x"), lax.axis_index("core")
    yl, z = lax.axis_index("yl"), lax.axis_index("z")
    shifts = [0, 1, nx - 1] + list(range(2, nx - 1))
    rows = latent_codes.shape[1]
    tokens = queries.shape[1]

    def by_core(core):
        blocks = []
        for array in (queries, out_grad):
            width = array.shape[2] // (2 * chips)
            block = array[0].reshape(tokens, ny, nx, 2, width)
            blocks.append(lax.dynamic_index_in_dim(block, core, 3, keepdims=False))
        return jnp.concatenate(blocks, axis=3)

    qg_away = by_core(1 - c)
    codes, qg_away = tie(latent_codes, qg_away)
    local = dequantize_columns(codes[0].T, exponents[0])
    both_y = jnp.concatenate([local, swap(local, "yh")], axis=1)
    qg = jnp.concatenate([by_core(c), swap(qg_away, "core")], axis=0)
    qg_parts = [lax.dynamic_index_in_dim(qg, lax.rem(x + b, nx), 2, keepdims=False) for b in shifts]
    both_y = tie(both_y, *qg_parts)[0]
    qg_parts = [lax.ppermute(part, "x", ring(nx, b)) if b else part for part, b in zip(qg_parts, shifts)]
    lat_parts = [lax.ppermute(both_y, "x", ring(nx, b)) if b else both_y for b in shifts]

    qg = jnp.concatenate(qg_parts, axis=0)
    qg_keep = lax.dynamic_index_in_dim(qg, y, 1, keepdims=False)
    qg_give = lax.dynamic_index_in_dim(qg, 1 - y, 1, keepdims=False)
    _, *lat_parts = tie(qg_give, *lat_parts)
    qg = jnp.concatenate([qg_keep, swap(qg_give, "yh")], axis=0)
    own = jnp.concatenate(lat_parts, axis=1)
    other = swap(own, "core")

    def row_starts(core):
        return [
            ((lax.rem(y + a, ny) * nx + lax.rem(x - b + nx, nx)) * 2 + core) * rows
            for b in shifts
            for a in range(ny)
        ]

    starts = jnp.stack(row_starts(c) + row_starts(1 - c))
    positions = (starts[:, None] + jnp.arange(rows, dtype=jnp.int32)[None, :]).reshape(1, -1)
    bias = jnp.where(positions < lengths[0], jnp.float32(0.0), -jnp.inf)

    pairs = w_key.shape[1] // (2 * PAIR * NOPE)
    *projected, q_columns, g_columns = project_call(qg, w_key, w_value)
    first = heads_call(bias, own, other, qg, projected, 0, pairs)
    second = heads_call(bias, own, other, qg, projected, pairs, pairs)

    nz = lax.axis_size("z")
    half = LATENT // 2
    keep = lax.dynamic_slice_in_dim(first[0], yl * half, half, 1)
    give = lax.dynamic_slice_in_dim(first[0], (1 - yl) * half, half, 1)
    sum_a = wide_add(keep, swap(give, "yl")).astype(bf16)
    shard = half // nz
    pieces_a = sum_a.reshape(2, nz, shard, -1)
    pieces_b = second[0].reshape(2, nz, 2 * shard, -1)

    def take(part):
        def of(offset):
            place = lax.rem(z + offset + nz, nz)
            return jnp.concatenate(
                [lax.dynamic_index_in_dim(p[part], place, 0, keepdims=False) for p in (pieces_a, pieces_b)],
                axis=0,
            )

        return of

    def row_grads(side):
        return lambda ready: latent_call((q_columns, g_columns), first, tie(second, ready)[0], side)

    pieces = []
    for part, fillers in enumerate(((row_grads(1), row_grads(0)), ())):
        summed, filled = reduce_ring(take(part), "z", fillers)
        if fillers:
            far, near = filled
        partner = swap(summed, "yl")
        sum_b = wide_add(summed[shard:], partner[shard:]).astype(bf16)
        pieces += gather_ring(jnp.concatenate([summed[:shard], partner[:shard], sum_b], axis=0), "z")

    pair_sum = wide_add(near, swap(far, "core")).astype(bf16)
    width = ny * rows
    back = []
    for k, b in enumerate(shifts):
        part = pair_sum[:, k * width : (k + 1) * width]
        back.append(lax.ppermute(part, "x", ring(nx, -b)) if b else part)
    row_sum = wide_add(*back)
    latent_grad = row_sum[:, :rows] + swap(row_sum[:, rows:].astype(bf16), "yh").astype(jnp.float32)

    key_sum, value_sum = assemble_call(jnp.stack([yl, z]).astype(jnp.int32), pieces)
    return (latent_grad.T[None], key_sum, value_sum)


def solution(mesh):
    devices = mesh.devices.reshape(2, 8, 2, 4, 2)
    split = Mesh(devices, ("yl", "z", "yh", "x", "core"))
    batch, head = ("yl", "z"), ("yh", "x", "core")
    in_specs = (
        P(batch, head, None),
        P(batch, head),
        P(batch),
        P(batch, head, None),
        P(batch, head, None),
        P(None, head),
        P(None, head),
    )
    out_specs = (P(batch, head, None), P(None, head), P(None, head))
    return jax.shard_map(
        per_device, mesh=split, in_specs=in_specs, out_specs=out_specs, check_vma=False
    )
```

```python
import functools

import jax
import jax.numpy as jnp
import numpy as np
from jax import lax
from jax.experimental import pallas as pl
from jax.experimental.pallas import tpu as pltpu
from jax.sharding import Mesh
from jax.sharding import PartitionSpec as P

LATENT = 512
ROPE = 64
NOPE = 128
VHEAD = 128
FEATURES = NOPE + ROPE
SCALE = FEATURES ** (-0.5)
LOG2E = float(np.log2(np.e))
QUERIES = 128
PAIR = 4
ROWS = PAIR * QUERIES
BLOCK = 16
LANES = 128
TILE = 256


lower_exponent = -9


def dequantize_columns(codes, exponents):
    levels = jnp.arange(5, dtype=jnp.int32) + lower_exponent
    powers = jnp.asarray(np.array([2.0**level for level in range(-9, -4)]), jnp.float32)
    factor = jnp.sum(jnp.where(exponents[..., None] == levels, powers, jnp.float32(0.0)), axis=-1)
    return (codes.astype(jnp.float32) * factor[None, :]).astype(jnp.bfloat16)


def dot_nn(left, right):
    return lax.dot_general(
        left, right, (((1,), (0,)), ((), ())), preferred_element_type=jnp.float32
    )


def dot_nt(left, right):
    return lax.dot_general(
        left, right, (((1,), (1,)), ((), ())), preferred_element_type=jnp.float32
    )


def project_kernel(qg_ref, wk_ref, wv_ref, qa_ref, ra_ref, ga_ref, qt_ref, gt_ref):
    bf16 = jnp.bfloat16
    eye = (
        lax.broadcasted_iota(jnp.int32, (ROPE, ROPE), 0)
        == lax.broadcasted_iota(jnp.int32, (ROPE, ROPE), 1)
    ).astype(jnp.float32).astype(bf16)
    pairs = wk_ref.shape[1] // (2 * NOPE)
    skip = wk_ref.shape[1] * FEATURES // NOPE

    def one_pair(pair, carry):
        def window(width, extra=0):
            return pl.ds(pl.multiple_of(extra + pair * width, 128), width)

        q_pair = qg_ref[:, window(2 * FEATURES)]
        for h in range(2):
            nope = q_pair[:, h * FEATURES : h * FEATURES + NOPE]
            rope = q_pair[:, h * FEATURES + NOPE : (h + 1) * FEATURES]
            head = pl.ds(pl.multiple_of((2 * pair + h) * NOPE, NOPE), NOPE)
            grad = qg_ref[:, pl.ds(pl.multiple_of(skip + (2 * pair + h) * VHEAD, VHEAD), VHEAD)]
            wk, wv = wk_ref[:, head], wv_ref[:, head]
            qa_ref[head, :] = dot_nt(nope, wk).astype(bf16)
            ra_ref[head, :] = rope
            ga_ref[head, :] = dot_nt(grad, wv).astype(bf16)
            qt_ref[:LATENT, head] = dot_nt(wk, nope).astype(bf16)
            qt_ref[LATENT:, head] = dot_nt(eye, rope).astype(bf16)
            gt_ref[:, head] = dot_nt(wv, grad).astype(bf16)
        return carry

    lax.fori_loop(0, pairs, one_pair, 0)


def project_call(qg, wk, wv):
    total = wk.shape[1] // NOPE * QUERIES
    vmem = pl.BlockSpec(memory_space=pltpu.VMEM)
    shapes = [(total, LATENT), (total, ROPE), (total, LATENT), (LATENT + ROPE, total), (LATENT, total)]
    return pl.pallas_call(
        project_kernel,
        in_specs=[vmem] * 3,
        out_specs=[vmem] * 5,
        out_shape=[jax.ShapeDtypeStruct(shape, jnp.bfloat16) for shape in shapes],
        compiler_params=pltpu.CompilerParams(vmem_limit_bytes=16 * 1024 * 1024),
        cost_estimate=pl.CostEstimate(
            flops=40 * 4 * total * NOPE * LATENT, bytes_accessed=8 * 1024 * 1024, transcendentals=0
        ),
        name="project",
    )(qg, wk, wv)


def heads_kernel(
    first, pairs,
    bias_ref, own_ref, other_ref, qg_ref, qa_ref, ra_ref, ga_ref,
    grads_ref, low_ref, ds_ref,
    scores_ref, gp_ref, top_ref, sum_ref, mix_ref,
):
    bf16 = jnp.bfloat16
    half = own_ref.shape[1]
    skip = qg_ref.shape[1] * FEATURES // (FEATURES + VHEAD)
    sides = ((own_ref, 0), (other_ref, half))

    def one_pair(pair, carry):
        def window(width, extra=0):
            return pl.ds(pl.multiple_of(extra + (first + pair) * width, 128), width)

        here = window(ROWS)
        q_all, r_all, g_all = qa_ref[here, :], ra_ref[here, :], ga_ref[here, :]
        for lat_ref, base in sides:

            def score_tile(step, carry, lat_ref=lat_ref, base=base):
                source = pl.ds(pl.multiple_of(step * TILE, TILE), TILE)
                columns = pl.ds(pl.multiple_of(base + step * TILE, TILE), TILE)
                main = lat_ref[:LATENT, source]
                total = dot_nn(q_all, main) + dot_nn(r_all, lat_ref[LATENT:, source])
                scores_ref[:, columns] = total * (SCALE * LOG2E) + bias_ref[:, columns]
                gp_ref[:, columns] = dot_nn(g_all, main)
                return carry

            lax.fori_loop(0, half // TILE, score_tile, 0)

        blocks = ROWS // BLOCK
        lanes = [slice(LANES * j, LANES * (j + 1)) for j in range(2 * half // LANES)]

        def row_block(step):
            return pl.ds(pl.multiple_of(step * BLOCK, BLOCK), BLOCK)

        def find_top(step, carry):
            rows = row_block(step)
            tops = [scores_ref[rows, lane] for lane in lanes]
            while len(tops) > 1:
                tops = [jnp.maximum(u, v) for u, v in zip(tops[::2], tops[1::2])]
            top_ref[rows, :] = tops[0]
            return carry

        lax.fori_loop(0, blocks, find_top, 0)
        top = jnp.max(top_ref[...], axis=1, keepdims=True)
        top_ref[...] = jnp.broadcast_to(top, top_ref.shape)

        def exponentiate(step, carry):
            rows = row_block(step)
            top = top_ref[rows, :]
            total = mixed = None
            for lane in lanes:
                expd = jnp.exp2(scores_ref[rows, lane] - top)
                scores_ref[rows, lane] = expd
                product = expd * gp_ref[rows, lane]
                total = expd if total is None else total + expd
                mixed = product if mixed is None else mixed + product
            sum_ref[rows, :] = total
            mix_ref[rows, :] = mixed
            return carry

        lax.fori_loop(0, blocks, exponentiate, 0, unroll=2)
        inverse = 1.0 / jnp.sum(sum_ref[...], axis=1, keepdims=True)
        out_dot = jnp.sum(mix_ref[...], axis=1, keepdims=True) * inverse
        sum_ref[...] = jnp.broadcast_to(inverse, sum_ref.shape)
        mix_ref[...] = jnp.broadcast_to(out_dot, mix_ref.shape)

        def finish(step, carry):
            rows = row_block(step)
            place = pl.ds(pl.multiple_of(pair * ROWS + step * BLOCK, BLOCK), BLOCK)
            inverse, out_dot = sum_ref[rows, :], mix_ref[rows, :]
            for lane in lanes:
                probs = scores_ref[rows, lane] * inverse
                low_ref[place, lane] = probs.astype(bf16)
                ds_ref[place, lane] = (probs * SCALE * (gp_ref[rows, lane] - out_dot)).astype(bf16)
            return carry

        lax.fori_loop(0, blocks, finish, 0, unroll=2)
        def back_pair(step, carry):
            local = pair * (PAIR // 2) + step
            rows = pl.ds(pl.multiple_of(local * 2 * QUERIES, 2 * QUERIES), 2 * QUERIES)
            place = first * (PAIR // 2) + local
            q_pair = qg_ref[:, pl.ds(pl.multiple_of(place * 2 * FEATURES, 128), 2 * FEATURES)]
            g_pair = qg_ref[:, pl.ds(pl.multiple_of(skip + place * 2 * VHEAD, 128), 2 * VHEAD)]

            def back(rows_ref):
                total = dot_nt(own_ref[:LATENT, :], rows_ref[rows, :half])
                return (total + dot_nt(other_ref[:LATENT, :], rows_ref[rows, half:])).astype(bf16)

            back_k, back_v = back(ds_ref), back(low_ref)
            for h in range(2):
                columns = slice(h * QUERIES, (h + 1) * QUERIES)
                head = pl.ds(pl.multiple_of((local * 2 + h) * NOPE, NOPE), NOPE)
                nope = q_pair[:, h * FEATURES : h * FEATURES + NOPE]
                grads_ref[0, :, head] = dot_nn(back_k[:, columns], nope).astype(bf16)
                grads_ref[1, :, head] = dot_nn(
                    back_v[:, columns], g_pair[:, h * VHEAD : (h + 1) * VHEAD]
                ).astype(bf16)
            return carry

        lax.fori_loop(0, PAIR // 2, back_pair, 0)
        return carry

    lax.fori_loop(0, pairs, one_pair, 0)


def heads_call(bias, own, other, qg, projected, first, pairs):
    total = pairs * ROWS
    prefix = 2 * own.shape[1]
    flops = 2 * total * prefix * LATENT * 4
    vmem = pl.BlockSpec(memory_space=pltpu.VMEM)
    return pl.pallas_call(
        functools.partial(heads_kernel, first, pairs),
        in_specs=[vmem] * 7,
        out_specs=[vmem] * 3,
        out_shape=[
            jax.ShapeDtypeStruct((2, LATENT, pairs * PAIR * NOPE), jnp.bfloat16),
            jax.ShapeDtypeStruct((total, prefix), jnp.bfloat16),
            jax.ShapeDtypeStruct((total, prefix), jnp.bfloat16),
        ],
        scratch_shapes=[
            pltpu.VMEM((ROWS, prefix), jnp.float32),
            pltpu.VMEM((ROWS, prefix), jnp.float32),
            pltpu.VMEM((ROWS, LANES), jnp.float32),
            pltpu.VMEM((ROWS, LANES), jnp.float32),
            pltpu.VMEM((ROWS, LANES), jnp.float32),
        ],
        compiler_params=pltpu.CompilerParams(vmem_limit_bytes=24 * 1024 * 1024),
        cost_estimate=pl.CostEstimate(
            flops=flops, bytes_accessed=8 * 1024 * 1024, transcendentals=total * prefix
        ),
        name="heads",
    )(bias, own, other, qg, *projected)


def latent_kernel(start, qt_ref, gt_ref, ds0_ref, ds1_ref, low0_ref, low1_ref, out_ref):
    tile = 256
    total = ds0_ref.shape[0]

    def one_tile(step, carry):
        source = pl.ds(pl.multiple_of(start + step * tile, tile), tile)
        place = pl.ds(pl.multiple_of(step * tile, tile), tile)
        ds0, ds1 = ds0_ref[:, source], ds1_ref[:, source]
        value = dot_nn(gt_ref[:, :total], low0_ref[:, source]) + dot_nn(
            gt_ref[:, total:], low1_ref[:, source]
        )
        key = dot_nn(qt_ref[:LATENT, :total], ds0) + dot_nn(qt_ref[:LATENT, total:], ds1)
        out_ref[:LATENT, place] = (value + key).astype(jnp.bfloat16)
        out_ref[LATENT:, place] = (
            dot_nn(qt_ref[LATENT:, :total], ds0) + dot_nn(qt_ref[LATENT:, total:], ds1)
        ).astype(jnp.bfloat16)
        return carry

    lax.fori_loop(0, out_ref.shape[1] // tile, one_tile, 0)


def latent_call(transposed, first, second, side):
    (_, low0, ds0), (_, low1, ds1) = first, second
    prefix = low0.shape[1] // 2
    total = low0.shape[0]
    vmem = pl.BlockSpec(memory_space=pltpu.VMEM)
    return pl.pallas_call(
        functools.partial(latent_kernel, side * prefix),
        in_specs=[vmem] * 6,
        out_specs=vmem,
        out_shape=jax.ShapeDtypeStruct((LATENT + ROPE, prefix), jnp.bfloat16),
        compiler_params=pltpu.CompilerParams(vmem_limit_bytes=24 * 1024 * 1024),
        cost_estimate=pl.CostEstimate(
            flops=2 * 2 * 2 * total * prefix * LATENT, bytes_accessed=12 * 1024 * 1024, transcendentals=0
        ),
        name="latent_rows",
    )(*transposed, ds0, ds1, low0, low1)


OFFSETS = (0, 1, -1, 2, -2, 3, -3, 4)


def assemble_kernel(index_ref, *refs):
    side, place = index_ref[0], index_ref[1]
    depth = len(OFFSETS)
    shard = refs[0].shape[0] // 4
    width = refs[0].shape[1]
    for k, offset in enumerate(OFFSETS):
        z = lax.rem(place - offset + depth, depth)
        kept = pl.ds(pl.multiple_of((side * depth + z) * shard, shard), shard)
        given = pl.ds(pl.multiple_of(((1 - side) * depth + z) * shard, shard), shard)
        both = pl.ds(pl.multiple_of(z * 2 * shard, 2 * shard), 2 * shard)
        for part, out_ref in enumerate(refs[2 * depth :]):
            piece = refs[part * depth + k]
            out_ref[kept, :width] = piece[:shard, :].astype(jnp.float32)
            out_ref[given, :width] = piece[shard : 2 * shard, :].astype(jnp.float32)
            out_ref[both, width:] = piece[2 * shard :, :].astype(jnp.float32)


def assemble_call(place, pieces):
    vmem = pl.BlockSpec(memory_space=pltpu.VMEM)
    out = jax.ShapeDtypeStruct((LATENT, 2 * pieces[0].shape[1]), jnp.float32)
    return pl.pallas_call(
        assemble_kernel,
        in_specs=[pl.BlockSpec(memory_space=pltpu.SMEM)] + [vmem] * len(pieces),
        out_specs=[vmem, vmem],
        out_shape=[out, out],
        compiler_params=pltpu.CompilerParams(vmem_limit_bytes=16 * 1024 * 1024),
        cost_estimate=pl.CostEstimate(flops=1 << 20, bytes_accessed=6 * 1024 * 1024, transcendentals=0),
        name="assemble",
    )(place, *pieces)


def ring(size, shift):
    return [(i, (i + shift) % size) for i in range(size)]


def wide_add(*terms):
    total = terms[0].astype(jnp.float32)
    for term in terms[1:]:
        total = total + term.astype(jnp.float32)
    return total


def tie(value, *others):
    return lax.optimization_barrier((value, *others))


def reduce_ring(take, axis, fill):
    size = lax.axis_size(axis)
    ahead = size // 2
    behind = size - 1 - ahead
    right, left = take(ahead), take(-behind)
    for step in range(ahead):
        ready = right
        with jax.named_scope(f"sum_{step}"):
            right = lax.ppermute(right, axis, ring(size, 1))
            if step < behind:
                left = lax.ppermute(left, axis, ring(size, -1))
        right = fill(step, ready, right)
        if step < ahead - 1:
            right = wide_add(right, take(ahead - 1 - step)).astype(jnp.bfloat16)
        if step < behind - 1:
            left = wide_add(left, take(-behind + 1 + step)).astype(jnp.bfloat16)
    return wide_add(right, left, take(0)).astype(jnp.bfloat16)


def gather_ring(shard, axis, beside=None):
    size = lax.axis_size(axis)
    ahead = size // 2
    parts = {0: shard}
    right = left = shard
    for step in range(1, ahead + 1):
        with jax.named_scope(f"gather_{step}"):
            right = lax.ppermute(right, axis, ring(size, 1))
            parts[step] = right
            if step < ahead:
                left = lax.ppermute(left, axis, ring(size, -1))
                parts[-step] = left
        if step == 2 and beside is not None:
            right = tie(right, beside)[0]
    return [parts[offset] for offset in OFFSETS]


def swap(value, axis):
    return lax.ppermute(value, axis, ring(2, 1))


def per_device(latent_codes, exponents, lengths, queries, out_grad, w_key, w_value):
    bf16 = jnp.bfloat16
    ny, nx = lax.axis_size("yh"), lax.axis_size("x")
    chips = ny * nx
    y, x, c = lax.axis_index("yh"), lax.axis_index("x"), lax.axis_index("core")
    yl, z = lax.axis_index("yl"), lax.axis_index("z")
    shifts = [0, 1, nx - 1] + list(range(2, nx - 1))
    rows = latent_codes.shape[1]
    tokens = queries.shape[1]

    def by_core(core):
        blocks = []
        for array in (queries, out_grad):
            width = array.shape[2] // (2 * chips)
            block = array[0].reshape(tokens, ny, nx, 2, width)
            blocks.append(lax.dynamic_index_in_dim(block, core, 3, keepdims=False))
        return jnp.concatenate(blocks, axis=3)

    qg_away = by_core(1 - c)
    codes, qg_away = tie(latent_codes, qg_away)
    local = dequantize_columns(codes[0].T, exponents[0])
    both_y = jnp.concatenate([local, swap(local, "yh")], axis=1)
    qg = jnp.concatenate([by_core(c), swap(qg_away, "core")], axis=0)
    qg_parts = [lax.dynamic_index_in_dim(qg, lax.rem(x + b, nx), 2, keepdims=False) for b in shifts]
    both_y = tie(both_y, *qg_parts)[0]
    qg_parts = [lax.ppermute(part, "x", ring(nx, b)) if b else part for part, b in zip(qg_parts, shifts)]
    lat_parts = [lax.ppermute(both_y, "x", ring(nx, b)) if b else both_y for b in shifts]

    qg = jnp.concatenate(qg_parts, axis=0)
    qg_keep = lax.dynamic_index_in_dim(qg, y, 1, keepdims=False)
    qg_give = lax.dynamic_index_in_dim(qg, 1 - y, 1, keepdims=False)
    _, *lat_parts = tie(qg_give, *lat_parts)
    qg = jnp.concatenate([qg_keep, swap(qg_give, "yh")], axis=0)
    own = jnp.concatenate(lat_parts, axis=1)
    other = swap(own, "core")

    def row_starts(core):
        return [
            ((lax.rem(y + a, ny) * nx + lax.rem(x - b + nx, nx)) * 2 + core) * rows
            for b in shifts
            for a in range(ny)
        ]

    starts = jnp.stack(row_starts(c) + row_starts(1 - c))
    positions = (starts[:, None] + jnp.arange(rows, dtype=jnp.int32)[None, :]).reshape(1, -1)
    bias = jnp.where(positions < lengths[0], jnp.float32(0.0), -jnp.inf)

    pairs = w_key.shape[1] // (2 * PAIR * NOPE)
    *projected, q_columns, g_columns = project_call(qg, w_key, w_value)
    first = heads_call(bias, own, other, qg, projected, 0, pairs)
    second = heads_call(bias, own, other, qg, projected, pairs, pairs)

    nz = lax.axis_size("z")
    half = LATENT // 2
    keep = lax.dynamic_slice_in_dim(first[0], yl * half, half, 1)
    give = lax.dynamic_slice_in_dim(first[0], (1 - yl) * half, half, 1)
    far = latent_call((q_columns, g_columns), first, second, 1)
    given = tie(swap(give, "yl"), far)[0]
    sum_a = wide_add(keep, given).astype(bf16)
    shard = half // nz
    pieces_a = sum_a.reshape(2, nz, shard, -1)
    pieces_b = second[0].reshape(2, nz, 2 * shard, -1)

    def take(offset):
        place = lax.rem(z + offset + nz, nz)
        return jnp.concatenate(
            [lax.dynamic_index_in_dim(p, place, 1, keepdims=False) for p in (pieces_a, pieces_b)], axis=1
        )

    away = swap(far, "core")
    width = ny * rows

    def near_rows(ready):
        return latent_call((q_columns, g_columns), first, tie(second, ready)[0], 0)

    def pair_rows(ready):
        return wide_add(near, away).astype(bf16)

    filled = []

    def fill(step, ready, arrived):
        if step == 0:
            filled.append(near_rows(ready))
        elif step == 1:
            filled.append(wide_add(filled[0], away).astype(bf16))
        else:
            return arrived
        return tie(arrived, filled[-1])[0]

    summed = reduce_ring(take, "z", fill)
    pair_sum = filled[1]
    back = []
    for k, b in enumerate(shifts):
        part = pair_sum[:, k * width : (k + 1) * width]
        with jax.named_scope("rows_x"):
            back.append(lax.ppermute(part, "x", ring(nx, -b)) if b else part)
    row_sum = wide_add(*back)

    partner = swap(summed, "yl")
    sum_b = wide_add(summed[:, shard:], partner[:, shard:]).astype(bf16)
    whole = jnp.concatenate([summed[:, :shard], partner[:, :shard], sum_b], axis=1)
    with jax.named_scope("rows_y"):
        last = swap(row_sum[:, rows:].astype(bf16), "yh")
    latent_grad = row_sum[:, :rows] + last.astype(jnp.float32)
    pieces = []
    for part in range(2):
        pieces += gather_ring(whole[part], "z", row_sum if part == 0 else None)
    key_sum, value_sum = assemble_call(jnp.stack([yl, z]).astype(jnp.int32), pieces)
    return (latent_grad.T[None], key_sum, value_sum)


def solution(mesh):
    devices = mesh.devices.reshape(2, 8, 2, 4, 2)
    split = Mesh(devices, ("yl", "z", "yh", "x", "core"))
    batch, head = ("yl", "z"), ("yh", "x", "core")
    in_specs = (
        P(batch, head, None),
        P(batch, head),
        P(batch),
        P(batch, head, None),
        P(batch, head, None),
        P(None, head),
        P(None, head),
    )
    out_specs = (P(batch, head, None), P(None, head), P(None, head))
    return jax.shard_map(
        per_device, mesh=split, in_specs=in_specs, out_specs=out_specs, check_vma=False
    )
```

```python
import functools

import jax
import jax.numpy as jnp
import numpy as np
from jax import lax
from jax.experimental import pallas as pl
from jax.experimental.pallas import tpu as pltpu
from jax.sharding import Mesh
from jax.sharding import PartitionSpec as P

LATENT = 512
ROPE = 64
NOPE = 128
VHEAD = 128
FEATURES = NOPE + ROPE
SCALE = FEATURES ** (-0.5)
LOG2E = float(np.log2(np.e))
QUERIES = 128
PAIR = 4
ROWS = PAIR * QUERIES
BLOCK = 16
LANES = 128
TILE = 512


lower_exponent = -9


def dequantize_columns(codes, exponents):
    levels = jnp.arange(5, dtype=jnp.int32) + lower_exponent
    powers = jnp.asarray(np.array([2.0**level for level in range(-9, -4)]), jnp.float32)
    factor = jnp.sum(jnp.where(exponents[..., None] == levels, powers, jnp.float32(0.0)), axis=-1)
    return (codes.astype(jnp.float32) * factor[None, :]).astype(jnp.bfloat16)


def dot_nn(left, right):
    return lax.dot_general(
        left, right, (((1,), (0,)), ((), ())), preferred_element_type=jnp.float32
    )


def dot_nt(left, right):
    return lax.dot_general(
        left, right, (((1,), (1,)), ((), ())), preferred_element_type=jnp.float32
    )


def project_kernel(qg_ref, wk_ref, wv_ref, qa_ref, ra_ref, ga_ref, qt_ref, gt_ref):
    bf16 = jnp.bfloat16
    eye = (
        lax.broadcasted_iota(jnp.int32, (ROPE, ROPE), 0)
        == lax.broadcasted_iota(jnp.int32, (ROPE, ROPE), 1)
    ).astype(jnp.float32).astype(bf16)
    pairs = wk_ref.shape[1] // (2 * NOPE)
    skip = wk_ref.shape[1] * FEATURES // NOPE

    def one_pair(pair, carry):
        def window(width, extra=0):
            return pl.ds(pl.multiple_of(extra + pair * width, 128), width)

        q_pair = qg_ref[:, window(2 * FEATURES)]
        for h in range(2):
            nope = q_pair[:, h * FEATURES : h * FEATURES + NOPE]
            rope = q_pair[:, h * FEATURES + NOPE : (h + 1) * FEATURES]
            head = pl.ds(pl.multiple_of((2 * pair + h) * NOPE, NOPE), NOPE)
            grad = qg_ref[:, pl.ds(pl.multiple_of(skip + (2 * pair + h) * VHEAD, VHEAD), VHEAD)]
            wk, wv = wk_ref[:, head], wv_ref[:, head]
            qa_ref[head, :] = dot_nt(nope, wk).astype(bf16)
            ra_ref[head, :] = rope
            ga_ref[head, :] = dot_nt(grad, wv).astype(bf16)
            qt_ref[:LATENT, head] = dot_nt(wk, nope).astype(bf16)
            qt_ref[LATENT:, head] = dot_nt(eye, rope).astype(bf16)
            gt_ref[:, head] = dot_nt(wv, grad).astype(bf16)
        return carry

    lax.fori_loop(0, pairs, one_pair, 0)


def project_call(qg, wk, wv):
    total = wk.shape[1] // NOPE * QUERIES
    vmem = pl.BlockSpec(memory_space=pltpu.VMEM)
    shapes = [(total, LATENT), (total, ROPE), (total, LATENT), (LATENT + ROPE, total), (LATENT, total)]
    return pl.pallas_call(
        project_kernel,
        in_specs=[vmem] * 3,
        out_specs=[vmem] * 5,
        out_shape=[jax.ShapeDtypeStruct(shape, jnp.bfloat16) for shape in shapes],
        compiler_params=pltpu.CompilerParams(vmem_limit_bytes=16 * 1024 * 1024),
        cost_estimate=pl.CostEstimate(
            flops=40 * 4 * total * NOPE * LATENT, bytes_accessed=8 * 1024 * 1024, transcendentals=0
        ),
        name="project",
    )(qg, wk, wv)


def heads_kernel(
    first, pairs,
    bias_ref, own_ref, other_ref, qg_ref, qa_ref, ra_ref, ga_ref,
    grads_ref, low_ref, ds_ref,
    scores_ref, gp_ref, top_ref, sum_ref, mix_ref,
):
    bf16 = jnp.bfloat16
    half = own_ref.shape[1]
    skip = qg_ref.shape[1] * FEATURES // (FEATURES + VHEAD)
    sides = ((own_ref, 0), (other_ref, half))

    def one_pair(pair, carry):
        def window(width, extra=0):
            return pl.ds(pl.multiple_of(extra + (first + pair) * width, 128), width)

        here = window(ROWS)
        q_all, r_all, g_all = qa_ref[here, :], ra_ref[here, :], ga_ref[here, :]
        for lat_ref, base in sides:

            def score_tile(step, carry, lat_ref=lat_ref, base=base):
                source = pl.ds(pl.multiple_of(step * TILE, TILE), TILE)
                columns = pl.ds(pl.multiple_of(base + step * TILE, TILE), TILE)
                main = lat_ref[:LATENT, source]
                total = dot_nn(q_all, main) + dot_nn(r_all, lat_ref[LATENT:, source])
                scores_ref[:, columns] = total * (SCALE * LOG2E) + bias_ref[:, columns]
                gp_ref[:, columns] = dot_nn(g_all, main)
                return carry

            lax.fori_loop(0, half // TILE, score_tile, 0)

        blocks = ROWS // BLOCK
        lanes = [slice(LANES * j, LANES * (j + 1)) for j in range(2 * half // LANES)]

        def row_block(step):
            return pl.ds(pl.multiple_of(step * BLOCK, BLOCK), BLOCK)

        def find_top(step, carry):
            rows = row_block(step)
            tops = [scores_ref[rows, lane] for lane in lanes]
            while len(tops) > 1:
                tops = [jnp.maximum(u, v) for u, v in zip(tops[::2], tops[1::2])]
            top_ref[rows, :] = tops[0]
            return carry

        lax.fori_loop(0, blocks, find_top, 0)
        top = jnp.max(top_ref[...], axis=1, keepdims=True)
        top_ref[...] = jnp.broadcast_to(top, top_ref.shape)

        def exponentiate(step, carry):
            rows = row_block(step)
            top = top_ref[rows, :]
            total = mixed = None
            for lane in lanes:
                expd = jnp.exp2(scores_ref[rows, lane] - top)
                scores_ref[rows, lane] = expd
                product = expd * gp_ref[rows, lane]
                total = expd if total is None else total + expd
                mixed = product if mixed is None else mixed + product
            sum_ref[rows, :] = total
            mix_ref[rows, :] = mixed
            return carry

        lax.fori_loop(0, blocks, exponentiate, 0)
        inverse = 1.0 / jnp.sum(sum_ref[...], axis=1, keepdims=True)
        out_dot = jnp.sum(mix_ref[...], axis=1, keepdims=True) * inverse
        sum_ref[...] = jnp.broadcast_to(inverse, sum_ref.shape)
        mix_ref[...] = jnp.broadcast_to(out_dot, mix_ref.shape)

        def finish(step, carry):
            rows = row_block(step)
            place = pl.ds(pl.multiple_of(pair * ROWS + step * BLOCK, BLOCK), BLOCK)
            inverse, out_dot = sum_ref[rows, :], mix_ref[rows, :]
            for lane in lanes:
                probs = scores_ref[rows, lane] * inverse
                low_ref[place, lane] = probs.astype(bf16)
                ds_ref[place, lane] = (probs * SCALE * (gp_ref[rows, lane] - out_dot)).astype(bf16)
            return carry

        lax.fori_loop(0, blocks, finish, 0)
        def back_pair(step, carry):
            local = pair * (PAIR // 2) + step
            rows = pl.ds(pl.multiple_of(local * 2 * QUERIES, 2 * QUERIES), 2 * QUERIES)
            place = first * (PAIR // 2) + local
            q_pair = qg_ref[:, pl.ds(pl.multiple_of(place * 2 * FEATURES, 128), 2 * FEATURES)]
            g_pair = qg_ref[:, pl.ds(pl.multiple_of(skip + place * 2 * VHEAD, 128), 2 * VHEAD)]

            def back(rows_ref):
                total = dot_nt(own_ref[:LATENT, :], rows_ref[rows, :half])
                return (total + dot_nt(other_ref[:LATENT, :], rows_ref[rows, half:])).astype(bf16)

            back_k, back_v = back(ds_ref), back(low_ref)
            for h in range(2):
                columns = slice(h * QUERIES, (h + 1) * QUERIES)
                head = pl.ds(pl.multiple_of((local * 2 + h) * NOPE, NOPE), NOPE)
                nope = q_pair[:, h * FEATURES : h * FEATURES + NOPE]
                grads_ref[0, :, head] = dot_nn(back_k[:, columns], nope).astype(bf16)
                grads_ref[1, :, head] = dot_nn(
                    back_v[:, columns], g_pair[:, h * VHEAD : (h + 1) * VHEAD]
                ).astype(bf16)
            return carry

        lax.fori_loop(0, PAIR // 2, back_pair, 0)
        return carry

    lax.fori_loop(0, pairs, one_pair, 0)


def heads_call(bias, own, other, qg, projected, first, pairs):
    total = pairs * ROWS
    prefix = 2 * own.shape[1]
    flops = 2 * total * prefix * LATENT * 4
    vmem = pl.BlockSpec(memory_space=pltpu.VMEM)
    return pl.pallas_call(
        functools.partial(heads_kernel, first, pairs),
        in_specs=[vmem] * 7,
        out_specs=[vmem] * 3,
        out_shape=[
            jax.ShapeDtypeStruct((2, LATENT, pairs * PAIR * NOPE), jnp.bfloat16),
            jax.ShapeDtypeStruct((total, prefix), jnp.bfloat16),
            jax.ShapeDtypeStruct((total, prefix), jnp.bfloat16),
        ],
        scratch_shapes=[
            pltpu.VMEM((ROWS, prefix), jnp.float32),
            pltpu.VMEM((ROWS, prefix), jnp.float32),
            pltpu.VMEM((ROWS, LANES), jnp.float32),
            pltpu.VMEM((ROWS, LANES), jnp.float32),
            pltpu.VMEM((ROWS, LANES), jnp.float32),
        ],
        compiler_params=pltpu.CompilerParams(vmem_limit_bytes=24 * 1024 * 1024),
        cost_estimate=pl.CostEstimate(
            flops=flops, bytes_accessed=8 * 1024 * 1024, transcendentals=total * prefix
        ),
        name="heads",
    )(bias, own, other, qg, *projected)


def latent_kernel(start, qt_ref, gt_ref, ds0_ref, ds1_ref, low0_ref, low1_ref, out_ref):
    tile = 256
    total = ds0_ref.shape[0]

    def one_tile(step, carry):
        source = pl.ds(pl.multiple_of(start + step * tile, tile), tile)
        place = pl.ds(pl.multiple_of(step * tile, tile), tile)
        ds0, ds1 = ds0_ref[:, source], ds1_ref[:, source]
        value = dot_nn(gt_ref[:, :total], low0_ref[:, source]) + dot_nn(
            gt_ref[:, total:], low1_ref[:, source]
        )
        key = dot_nn(qt_ref[:LATENT, :total], ds0) + dot_nn(qt_ref[:LATENT, total:], ds1)
        out_ref[:LATENT, place] = (value + key).astype(jnp.bfloat16)
        out_ref[LATENT:, place] = (
            dot_nn(qt_ref[LATENT:, :total], ds0) + dot_nn(qt_ref[LATENT:, total:], ds1)
        ).astype(jnp.bfloat16)
        return carry

    lax.fori_loop(0, out_ref.shape[1] // tile, one_tile, 0)


def latent_call(transposed, first, second, side):
    (_, low0, ds0), (_, low1, ds1) = first, second
    prefix = low0.shape[1] // 2
    total = low0.shape[0]
    vmem = pl.BlockSpec(memory_space=pltpu.VMEM)
    return pl.pallas_call(
        functools.partial(latent_kernel, side * prefix),
        in_specs=[vmem] * 6,
        out_specs=vmem,
        out_shape=jax.ShapeDtypeStruct((LATENT + ROPE, prefix), jnp.bfloat16),
        compiler_params=pltpu.CompilerParams(vmem_limit_bytes=24 * 1024 * 1024),
        cost_estimate=pl.CostEstimate(
            flops=2 * 2 * 2 * total * prefix * LATENT, bytes_accessed=12 * 1024 * 1024, transcendentals=0
        ),
        name="latent_rows",
    )(*transposed, ds0, ds1, low0, low1)


OFFSETS = (0, 1, -1, 2, -2, 3, -3, 4)


def assemble_kernel(index_ref, *refs):
    side, place = index_ref[0], index_ref[1]
    depth = len(OFFSETS)
    shard = refs[0].shape[0] // 4
    width = refs[0].shape[1]
    for k, offset in enumerate(OFFSETS):
        z = lax.rem(place - offset + depth, depth)
        kept = pl.ds(pl.multiple_of((side * depth + z) * shard, shard), shard)
        given = pl.ds(pl.multiple_of(((1 - side) * depth + z) * shard, shard), shard)
        both = pl.ds(pl.multiple_of(z * 2 * shard, 2 * shard), 2 * shard)
        for part, out_ref in enumerate(refs[2 * depth :]):
            piece = refs[part * depth + k]
            out_ref[kept, :width] = piece[:shard, :].astype(jnp.float32)
            out_ref[given, :width] = piece[shard : 2 * shard, :].astype(jnp.float32)
            out_ref[both, width:] = piece[2 * shard :, :].astype(jnp.float32)


def assemble_call(place, pieces):
    vmem = pl.BlockSpec(memory_space=pltpu.VMEM)
    out = jax.ShapeDtypeStruct((LATENT, 2 * pieces[0].shape[1]), jnp.float32)
    return pl.pallas_call(
        assemble_kernel,
        in_specs=[pl.BlockSpec(memory_space=pltpu.SMEM)] + [vmem] * len(pieces),
        out_specs=[vmem, vmem],
        out_shape=[out, out],
        compiler_params=pltpu.CompilerParams(vmem_limit_bytes=16 * 1024 * 1024),
        cost_estimate=pl.CostEstimate(flops=1 << 20, bytes_accessed=6 * 1024 * 1024, transcendentals=0),
        name="assemble",
    )(place, *pieces)


def ring(size, shift):
    return [(i, (i + shift) % size) for i in range(size)]


def wide_add(*terms):
    total = terms[0].astype(jnp.float32)
    for term in terms[1:]:
        total = total + term.astype(jnp.float32)
    return total


def tie(value, *others):
    return lax.optimization_barrier((value, *others))


def reduce_ring(take, axis, fill):
    size = lax.axis_size(axis)
    ahead = size // 2
    behind = size - 1 - ahead
    right, left = take(ahead), take(-behind)
    for step in range(ahead):
        ready = right
        with jax.named_scope(f"sum_{step}"):
            right = lax.ppermute(right, axis, ring(size, 1))
            if step < behind:
                left = lax.ppermute(left, axis, ring(size, -1))
        right = fill(step, ready, right)
        if step < ahead - 1:
            right = wide_add(right, take(ahead - 1 - step)).astype(jnp.bfloat16)
        if step < behind - 1:
            left = wide_add(left, take(-behind + 1 + step)).astype(jnp.bfloat16)
    return wide_add(right, left, take(0)).astype(jnp.bfloat16)


def gather_ring(shard, axis, beside=None):
    size = lax.axis_size(axis)
    ahead = size // 2
    parts = {0: shard}
    right = left = shard
    for step in range(1, ahead + 1):
        with jax.named_scope(f"gather_{step}"):
            right = lax.ppermute(right, axis, ring(size, 1))
            parts[step] = right
            if step < ahead:
                left = lax.ppermute(left, axis, ring(size, -1))
                parts[-step] = left
        if step == 2 and beside is not None:
            right = tie(right, beside)[0]
    return [parts[offset] for offset in OFFSETS]


def swap(value, axis):
    return lax.ppermute(value, axis, ring(2, 1))


def per_device(latent_codes, exponents, lengths, queries, out_grad, w_key, w_value):
    bf16 = jnp.bfloat16
    ny, nx = lax.axis_size("yh"), lax.axis_size("x")
    chips = ny * nx
    y, x, c = lax.axis_index("yh"), lax.axis_index("x"), lax.axis_index("core")
    yl, z = lax.axis_index("yl"), lax.axis_index("z")
    shifts = [0, 1, nx - 1] + list(range(2, nx - 1))
    rows = latent_codes.shape[1]
    tokens = queries.shape[1]

    def by_core(core):
        blocks = []
        for array in (queries, out_grad):
            width = array.shape[2] // (2 * chips)
            block = array[0].reshape(tokens, ny, nx, 2, width)
            blocks.append(lax.dynamic_index_in_dim(block, core, 3, keepdims=False))
        return jnp.concatenate(blocks, axis=3)

    qg_away = by_core(1 - c)
    codes, qg_away = tie(latent_codes, qg_away)
    local = dequantize_columns(codes[0].T, exponents[0])
    both_y = jnp.concatenate([local, swap(local, "yh")], axis=1)
    qg = jnp.concatenate([by_core(c), swap(qg_away, "core")], axis=0)
    qg_parts = [lax.dynamic_index_in_dim(qg, lax.rem(x + b, nx), 2, keepdims=False) for b in shifts]
    both_y = tie(both_y, *qg_parts)[0]
    qg_parts = [lax.ppermute(part, "x", ring(nx, b)) if b else part for part, b in zip(qg_parts, shifts)]
    lat_parts = [lax.ppermute(both_y, "x", ring(nx, b)) if b else both_y for b in shifts]

    qg = jnp.concatenate(qg_parts, axis=0)
    qg_keep = lax.dynamic_index_in_dim(qg, y, 1, keepdims=False)
    qg_give = lax.dynamic_index_in_dim(qg, 1 - y, 1, keepdims=False)
    _, *lat_parts = tie(qg_give, *lat_parts)
    qg = jnp.concatenate([qg_keep, swap(qg_give, "yh")], axis=0)
    own = jnp.concatenate(lat_parts, axis=1)
    other = swap(own, "core")

    def row_starts(core):
        return [
            ((lax.rem(y + a, ny) * nx + lax.rem(x - b + nx, nx)) * 2 + core) * rows
            for b in shifts
            for a in range(ny)
        ]

    starts = jnp.stack(row_starts(c) + row_starts(1 - c))
    positions = (starts[:, None] + jnp.arange(rows, dtype=jnp.int32)[None, :]).reshape(1, -1)
    bias = jnp.where(positions < lengths[0], jnp.float32(0.0), -jnp.inf)

    pairs = w_key.shape[1] // (2 * PAIR * NOPE)
    *projected, q_columns, g_columns = project_call(qg, w_key, w_value)
    first = heads_call(bias, own, other, qg, projected, 0, pairs)
    second = heads_call(bias, own, other, qg, projected, pairs, pairs)

    nz = lax.axis_size("z")
    half = LATENT // 2
    keep = lax.dynamic_slice_in_dim(first[0], yl * half, half, 1)
    give = lax.dynamic_slice_in_dim(first[0], (1 - yl) * half, half, 1)
    far = latent_call((q_columns, g_columns), first, second, 1)
    given = tie(swap(give, "yl"), far)[0]
    sum_a = wide_add(keep, given).astype(bf16)
    shard = half // nz
    pieces_a = sum_a.reshape(2, nz, shard, -1)
    pieces_b = second[0].reshape(2, nz, 2 * shard, -1)

    def take(offset):
        place = lax.rem(z + offset + nz, nz)
        return jnp.concatenate(
            [lax.dynamic_index_in_dim(p, place, 1, keepdims=False) for p in (pieces_a, pieces_b)], axis=1
        )

    away = swap(far, "core")
    width = ny * rows

    def near_rows(ready):
        return latent_call((q_columns, g_columns), first, tie(second, ready)[0], 0)

    def pair_rows(ready):
        return wide_add(near, away).astype(bf16)

    filled = []

    def fill(step, ready, arrived):
        if step == 0:
            filled.append(near_rows(ready))
        elif step == 1:
            filled.append(wide_add(filled[0], away).astype(bf16))
        else:
            return arrived
        return tie(arrived, filled[-1])[0]

    summed = reduce_ring(take, "z", fill)
    pair_sum = filled[1]
    back = []
    for k, b in enumerate(shifts):
        part = pair_sum[:, k * width : (k + 1) * width]
        with jax.named_scope("rows_x"):
            back.append(lax.ppermute(part, "x", ring(nx, -b)) if b else part)
    row_sum = wide_add(*back)

    partner = swap(summed, "yl")
    sum_b = wide_add(summed[:, shard:], partner[:, shard:]).astype(bf16)
    whole = jnp.concatenate([summed[:, :shard], partner[:, :shard], sum_b], axis=1)
    with jax.named_scope("rows_y"):
        last = swap(row_sum[:, rows:].astype(bf16), "yh")
    latent_grad = row_sum[:, :rows] + last.astype(jnp.float32)
    pieces = []
    for part in range(2):
        pieces += gather_ring(whole[part], "z", row_sum if part == 0 else None)
    key_sum, value_sum = assemble_call(jnp.stack([yl, z]).astype(jnp.int32), pieces)
    return (latent_grad.T[None], key_sum, value_sum)


def solution(mesh):
    devices = mesh.devices.reshape(2, 8, 2, 4, 2)
    split = Mesh(devices, ("yl", "z", "yh", "x", "core"))
    batch, head = ("yl", "z"), ("yh", "x", "core")
    in_specs = (
        P(batch, head, None),
        P(batch, head),
        P(batch),
        P(batch, head, None),
        P(batch, head, None),
        P(None, head),
        P(None, head),
    )
    out_specs = (P(batch, head, None), P(None, head), P(None, head))
    return jax.shard_map(
        per_device, mesh=split, in_specs=in_specs, out_specs=out_specs, check_vma=False
    )
```
